256 devices in a mesh: seq: 64 (over z, y, core), feat: 4 (over x).
Axes of the slice: x: 4, y: 4, z: 8, core: 2. Of those that a mesh axis runs over, the one named last changes fastest.
Arguments:
- hidden_in: bfloat16 [4, 16384, 2048], P(None, 'seq'), may hold values from -6 to 6
- w_query: bfloat16 [2048, 256], replicated, may hold values from -0.125 to 0.125
- w_key: bfloat16 [2048, 256], replicated, may hold values from -0.125 to 0.125
- w_value: bfloat16 [2048, 2048], P(None, 'feat'), may hold values from -0.125 to 0.125
- lengths: int32 [4], replicated, may hold values from 8192 to 16384, as said below
- owners: int32 [4], replicated, may hold values from 0 to 63
Outputs:
- mixed: bfloat16 [4, 16384, 2048], P(None, 'seq', 'feat')
- state_quad: float32 [64, 4, 16, 256, 128], P('seq', None, None, 'feat')
- state_low: float32 [64, 4, 16, 17, 128], P('seq', None, 'feat')
- norm_quad: float32 [64, 4, 16, 256], P('seq', None, None, 'feat')
- norm_low: float32 [64, 4, 16, 17], P('seq', None, 'feat')
The draws below stay inside these ranges and needn't reach their ends.
Inputs may be any that keep to these rules, and one draw needn't show every extreme that they name: `lengths`: every prompt holds 8192 to 16384 live tokens, and some prompt holds exactly 16384. `owners`: several prompts may share a decoding device.
All inputs are finite; a program needn't handle non-finite values.
Results may differ from the reference program's by a relative error of at most 0.0085.
Values may be sent and summed in bfloat16 or wider, within the bound.
No kernel may reach another device: no remote copies, remote signals or barrier semaphores. Data moves between devices by JAX's collectives and lax.ppermute only.
A program may use at most 256 MiB of HBM per device.

```python
import jax
import jax.numpy as jnp
from jax import lax

D = 2048
H = 16
HD = 128
FD = 16
PROMPTS = 4
SPAN = 256
LENGTH = 16384
N_SEQ = 64


def draw_lengths(key, part):
    first_key, second_key = jax.random.split(jax.random.fold_in(key, 11))
    drawn = jax.random.randint(first_key, (PROMPTS,), LENGTH // 2, LENGTH + 1)
    longest = jax.random.randint(second_key, (), 0, PROMPTS)
    return jnp.where(jnp.arange(PROMPTS) == longest, LENGTH, drawn).astype(jnp.int32)


def touch_ends(array, stream_key, least, top_value):
    dims = array.shape
    spot = [jax.random.randint(jax.random.fold_in(stream_key, axis), (), 0, dims[axis]) for axis in range(len(dims))]
    array = array.at[tuple(spot)].set(least)
    longest = dims.index(max(dims))
    spot[longest] = (spot[longest] + 1) % dims[longest]
    return array.at[tuple(spot)].set(top_value)


def levels(stream_key, shape, shards, low, largest):
    def one(axis_at, parts):
        draws = jax.random.uniform(jax.random.fold_in(jax.random.fold_in(stream_key, 6), axis_at), (parts,), jnp.float32, low / len(shards), largest / len(shards))
        return jnp.repeat(jnp.exp(draws), shape[axis_at] // parts).reshape((-1,) + (1,) * (len(shape) - axis_at - 1))

    level = one(*shards[0])
    for cut in shards[1:]:
        level = level * one(*cut)
    return level


def noise(own_key, shape, spread, most, cuts=(), held_as=jnp.bfloat16):
    array = jax.random.normal(own_key, shape, jnp.float32) * spread
    if len(cuts) > 0:
        array = levels(own_key, shape, cuts, -0.22, 0.18) * array
    return jnp.clip(array, min=-most, max=most).astype(held_as)


def setup_inputs(seed: int = 0) -> dict:
    streams_of = jax.random.split(jax.random.key(seed), 7)
    hidden_in = noise(streams_of[0], (PROMPTS, LENGTH, D), 1.0, 6.0, ((1, 64),))
    w_query = noise(streams_of[1], (D, H * FD), D ** -0.5, 0.125)
    w_key = noise(streams_of[2], (D, H * FD), D ** -0.5, 0.125)
    w_value = noise(streams_of[3], (D, D), D ** -0.5, 0.125, ((1, 4),))
    lengths = draw_lengths(jax.random.fold_in(streams_of[6], 71), 0)
    owners = touch_ends(jax.random.randint(streams_of[5], (PROMPTS,), 0, N_SEQ), jax.random.fold_in(streams_of[5], 1), 0, N_SEQ - 1).astype(jnp.int32)
    return dict(hidden_in=hidden_in, w_query=w_query, w_key=w_key, w_value=w_value, lengths=lengths, owners=owners)


NORM_FLOOR = 0.0001

def low_features(inputs):
    constant = jnp.ones(inputs.shape[:-1] + (1,), jnp.float32)
    return jnp.concatenate([constant, inputs * FD ** (-0.25)], axis=-1)

def quad_features(leading, inputs):
    products = leading[..., :, None] * inputs[..., None, :]
    return products.reshape(inputs.shape[:-1] + (leading.shape[-1] * inputs.shape[-1],)) * (2.0 * FD) ** (-0.5)

def reference(hidden_in, w_query, w_key, w_value, lengths, owners):
    highest = lax.Precision.HIGHEST
    n_blocks = LENGTH // SPAN

    def per_prompt(prompt_item):
        tokens, length = prompt_item
        queries = jnp.dot(tokens, w_query, preferred_element_type=jnp.float32).astype(jnp.bfloat16)
        key_rows = jnp.dot(tokens, w_key, preferred_element_type=jnp.float32).astype(jnp.bfloat16)
        values = jnp.dot(tokens, w_value, preferred_element_type=jnp.float32).astype(jnp.bfloat16)
        query_blocks = queries.astype(jnp.float32).reshape(n_blocks, SPAN, H, FD)
        key_blocks = key_rows.astype(jnp.float32).reshape(n_blocks, SPAN, H, FD)
        value_blocks = values.astype(jnp.float32).reshape(n_blocks, SPAN, H, HD)
        starts = jnp.arange(n_blocks, dtype=jnp.int32) * SPAN
        causal = (jnp.arange(SPAN)[:, None] >= jnp.arange(SPAN)[None, :]).astype(jnp.float32)

        def advance(carried, block_data):
            state_lo, state_qu, norm_lo, norm_qu = carried
            query_blk, key_blk, value_blk, start = block_data
            positions = start + jnp.arange(SPAN, dtype=jnp.int32)
            live_mask = (positions < length).astype(jnp.float32)
            query_low = low_features(query_blk)
            query_quad = quad_features(query_blk, query_blk)
            key_low = low_features(key_blk) * live_mask[:, None, None]
            key_quad = quad_features(key_blk, key_blk) * live_mask[:, None, None]
            numerator = jnp.einsum('thf,hfd->thd', query_low, state_lo, precision=highest)
            numerator = numerator + jnp.einsum('thf,hfd->thd', query_quad, state_qu, precision=highest)
            denominator = jnp.einsum('thf,hf->th', query_low, norm_lo, precision=highest)
            denominator = denominator + jnp.einsum('thf,hf->th', query_quad, norm_qu, precision=highest)
            scores = jnp.einsum('thf,uhf->htu', query_blk, key_blk, precision=highest)
            kernel = 1.0 + scores * FD ** (-0.5) + scores * scores * (0.5 / FD)
            weight = kernel * causal[None, :, :] * live_mask[None, None, :]
            numerator = numerator + jnp.einsum('htu,uhd->thd', weight, value_blk, precision=highest)
            denominator = denominator + lax.optimization_barrier(jnp.sum(weight, axis=2)).T
            attended = numerator / denominator[:, :, None] * live_mask[:, None, None]
            new_carried = (state_lo + jnp.einsum('thf,thd->hfd', key_low, value_blk, precision=highest), state_qu + jnp.einsum('thf,thd->hfd', key_quad, value_blk, precision=highest), norm_lo + lax.optimization_barrier(jnp.sum(key_low, axis=0)), norm_qu + lax.optimization_barrier(jnp.sum(key_quad, axis=0)))
            return (new_carried, attended.reshape(SPAN, H * HD))
        initial = (jnp.zeros((H, FD + 1, HD), jnp.float32), jnp.zeros((H, FD * FD, HD), jnp.float32), jnp.zeros((H, FD + 1), jnp.float32), jnp.zeros((H, FD * FD), jnp.float32))
        finals, attended = lax.scan(advance, initial, (query_blocks, key_blocks, value_blocks, starts))
        attended = attended.reshape(LENGTH, H * HD)
        mean_square = lax.optimization_barrier(jnp.mean(attended * attended, axis=-1))
        mixed = (attended * lax.rsqrt(mean_square + NORM_FLOOR)[:, None]).astype(jnp.bfloat16)
        return (mixed, finals)
    mixed, finals = lax.map(per_prompt, (hidden_in, lengths))
    final_low, final_quad, final_lnorm, final_qnorm = finals
    owner_table = (jnp.arange(N_SEQ, dtype=jnp.int32)[:, None] == owners[None, :]).astype(jnp.float32)
    state_quad = owner_table[:, :, None, None, None] * final_quad[None]
    state_low = owner_table[:, :, None, None, None] * final_low[None]
    norm_quad = owner_table[:, :, None, None] * final_qnorm[None]
    norm_low = owner_table[:, :, None, None] * final_lnorm[None]
    return (mixed, state_quad, state_low, norm_quad, norm_low)
```

```python
import functools

import jax
import jax.numpy as jnp
import numpy as np
from jax import lax
from jax.experimental import pallas as pl
from jax.experimental.pallas import tpu as pltpu
from jax.sharding import Mesh
from jax.sharding import PartitionSpec as P

H = 16
FD = 16
HD = 128
D = 2048
SPAN = 256
OWN = 4
ROWS = 160
QUADS = 136
LOW = 128
NORM = 153
CHIPS = 32
SLICE = 2 * OWN * ROWS // CHIPS
NORM_FLOOR = 0.0001
BF = jnp.bfloat16
F32 = jnp.float32
CHIP = ("z", "y")


def feature_rows():
    pairs = [(i, j) for i in range(FD) for j in range(i, FD)]
    rows = [u if u < LOW else u + FD + 1 for u in range(QUADS)]
    return pairs, rows


def tables():
    pairs, rows = feature_rows()
    first = np.zeros((ROWS, FD), np.float32)
    second = np.zeros((ROWS, FD), np.float32)
    spread = np.zeros((FD * FD, ROWS), np.float32)
    for (i, j), row in zip(pairs, rows):
        first[row, i] = 1
        second[row, j] = 1
        spread[i * FD + j, row] = 1
        spread[j * FD + i, row] = 1
    for i in range(FD):
        first[LOW + 1 + i, i] = 1
    picks = np.zeros((2, 2, OWN, ROWS, 2 * OWN * FD), np.float32)
    for half in range(2):
        for head in range(OWN):
            at = half * OWN * FD + head * FD
            picks[half, 0, head, :, at : at + FD] = first
            picks[half, 1, head, :, at : at + FD] = second
    lines = np.zeros((8, ROWS), np.float32)
    for (i, j), row in zip(pairs, rows):
        lines[0, row] = (1.0 if i == j else 2.0) * (2.0 * FD) ** -0.5
    lines[0, LOW + 1 : LOW + 1 + FD] = lines[1, LOW + 1 : LOW + 1 + FD] = FD**-0.25
    lines[:3, LOW] = 1.0
    return picks.reshape(2, 2, OWN * ROWS, 2 * OWN * FD), spread, lines


PICKS, SPREAD, LINES = tables()


def is_low(row):
    return (row >= LOW) & (row <= LOW + FD)


def nt(a, b):
    return lax.dot_general(a, b, (((1,), (1,)), ((), ())), preferred_element_type=F32)


def project_kernel(s, hid, wv, wq, wk, picks, q_o, k_o, v_o, send_o, keep_o, wqk):
    step = pl.program_id(0)
    local = (step + 2) % 4

    @pl.when(step == 0)
    def _():
        wqk[:, :128] = wq[...]
        wqk[:, 128:] = wk[...]

    x = hid[0]
    qk = jnp.dot(x, wqk[...], preferred_element_type=F32)
    v = jnp.dot(x, wv[...], preferred_element_type=F32).astype(BF)
    v_o[0] = v
    q_o[0] = qk[:, :128].astype(BF)
    key = qk[:, 128:].astype(BF)
    k_o[0] = key
    key_t = key.astype(F32).T.astype(BF)
    token = s[2] * SPAN + lax.broadcasted_iota(jnp.int32, (1, SPAN), 1)
    live = (token < s[3 + local]).astype(F32)
    row = lax.broadcasted_iota(jnp.int32, (ROWS, SPAN), 0)
    low = is_low(row)
    const = (row == LOW).astype(F32)
    scale = jnp.where(row == LOW, 1.0, jnp.where(low, FD**-0.25, (2.0 * FD) ** -0.5)) * live
    bias = jnp.where(low, scale, 0.0)
    ones = jnp.ones((8, SPAN), BF)
    tail_row = lax.broadcasted_iota(jnp.int32, (8, HD), 0) + (ROWS - 8)
    for h in range(OWN):
        at = h * ROWS
        u = jnp.dot(picks[0, 0, at : at + ROWS], key_t, preferred_element_type=F32)
        w = jnp.dot(picks[0, 1, at : at + ROWS], key_t, preferred_element_type=F32)
        feats = ((u + const) * (w * scale + bias)).astype(BF)
        state = jnp.dot(feats, v[:, h * HD : (h + 1) * HD], preferred_element_type=F32)
        norm = nt(ones, feats)
        rest = jnp.concatenate([norm[:, HD:], jnp.zeros((8, 2 * HD - ROWS), F32)], axis=1)
        tail = state[ROWS - 8 :]
        tail = jnp.where(tail_row == NORM, norm[:, :HD], jnp.where(tail_row == NORM + 1, rest, tail))
        packed = jnp.concatenate([state[: ROWS - 8], tail], axis=0).astype(BF)

        @pl.when(step < 2)
        def _():
            send_o[0, at : at + ROWS] = packed

        @pl.when(step >= 2)
        def _():
            keep_o[0, at : at + ROWS] = packed


def self_kernel(s, q, k, v, picks, lines, num_o, den_o, feat_o):
    local = pl.program_id(0)
    query, key, value = q[0], k[0], v[0]
    tq = lax.broadcasted_iota(jnp.int32, (SPAN, SPAN), 0)
    tk = lax.broadcasted_iota(jnp.int32, (SPAN, SPAN), 1)
    seen = (tk <= tq) & (s[2] * SPAN + tk < s[3 + local])
    lane = lax.broadcasted_iota(jnp.int32, (SPAN, HD), 1)
    scale, bias, const = lines[0:1], lines[1:2], lines[2:3]
    ones = jnp.ones((SPAN, HD), BF)
    den_all = jnp.zeros((SPAN, HD), F32)
    for h in range(OWN):
        at = h * ROWS
        mine = jnp.where(lane // FD == s[1] * OWN + h, query, jnp.zeros_like(query))
        score = nt(mine, key)
        weight = jnp.where(seen, 1.0 + score * (FD**-0.5) + score * score * (0.5 / FD), 0.0).astype(BF)
        num_o[0, :, h * HD : (h + 1) * HD] = jnp.dot(
            weight, value[:, h * HD : (h + 1) * HD], preferred_element_type=F32
        )
        den = jnp.dot(weight, ones, preferred_element_type=F32)
        den_all = jnp.where(lane == h, den, den_all)
        u = nt(query, picks[0, 0, at : at + ROWS])
        w = nt(query, picks[0, 1, at : at + ROWS])
        feat_o[0, h] = ((u + const) * (w * scale + bias)).astype(BF)
    den_o[0] = den_all


def scan_kernel(s, pieces, out):
    before = jnp.zeros((SLICE, HD), F32)
    for chip in range(CHIPS):
        out[chip, :SLICE] = before.astype(BF)
        before = before + pieces[chip].astype(F32)
    total = before.astype(BF)
    nothing = jnp.zeros_like(total)
    for chip in range(CHIPS):
        out[chip, SLICE:] = jnp.where(s[7] == chip, total, nothing)


def prefix_kernel(s, back, keep, recv, own_o, other_o):
    before = back[...].reshape(2 * OWN * ROWS, HD).astype(F32)
    second = s[0] == 1
    added = jnp.where(second, recv[...], keep[...]).reshape(2 * OWN * ROWS, HD).astype(F32)
    both = (before + added).astype(BF)
    plain = before.astype(BF)
    own_o[...] = jnp.where(second, both, plain).reshape(2, OWN * ROWS, HD)
    other_o[...] = jnp.where(second, plain, both).reshape(2, OWN * ROWS, HD)


def spread_kernel(back, spread, out, low_o):
    total = back[...].reshape(2 * OWN, ROWS, HD)
    low_o[...] = total[:, LOW:]
    rows = []
    for n in range(2 * OWN):
        wide = jnp.dot(spread[...], total[n], preferred_element_type=F32).astype(BF)
        for f in range(4):
            out[f, n * 64 : (n + 1) * 64] = wide[f * 64 : (f + 1) * 64]
        rows.append(
            jnp.concatenate(
                [total[n, NORM : NORM + 1], total[n, NORM + 1 : NORM + 2, : ROWS - HD]], axis=1
            )
        )
    norm = nt(jnp.concatenate(rows, axis=0), spread[...])
    pad = jnp.zeros((8, 64), F32)
    for f in range(4):
        out[f, 512:] = jnp.concatenate([norm[:, f * 64 : (f + 1) * 64], pad], axis=1).astype(BF)


def attend_kernel(s, first, state, num, den, feat, att_o, square_o):
    step = pl.program_id(0)
    lane = lax.broadcasted_iota(jnp.int32, (SPAN, HD), 1)
    token = s[2] * SPAN + lax.broadcasted_iota(jnp.int32, (SPAN, HD), 0)
    live = token < s[3 + first + step]
    den_all = den[0]
    squares = jnp.zeros((SPAN, HD), F32)
    for h in range(OWN):
        feats = feat[0, h]
        part = state[0, h * ROWS : (h + 1) * ROWS]
        norm = jnp.concatenate([part[NORM : NORM + 1], part[NORM + 1 : NORM + 2, : ROWS - HD]], axis=1)
        total = num[0, :, h * HD : (h + 1) * HD] + jnp.dot(feats, part, preferred_element_type=F32)
        below = nt(feats, jnp.broadcast_to(norm, (HD, ROWS))) + den_all[:, h : h + 1]
        att = jnp.where(live, total / below, 0.0)
        att_o[0, :, h * HD : (h + 1) * HD] = att
        squares = squares + att * att
    ones = jnp.ones((8, HD), F32)
    square_o[0] = lax.dot_general(
        ones, squares, (((1,), (1,)), ((), ())), precision=lax.Precision.HIGHEST, preferred_element_type=F32
    )


def mix_kernel(s, own, other, square, mixed_o):
    step = pl.program_id(0)
    factor = lax.rsqrt(square[0] * (1.0 / D) + NORM_FLOOR)
    column = factor.T[:, :1]

    @pl.when(step < 2)
    def _():
        mixed_o[0] = (own[0] * column).astype(BF)

    @pl.when(step >= 2)
    def _():
        mixed_o[0] = (other[0] * column).astype(BF)


def final_kernel(s, mine, theirs, low_mine, low_theirs, quad_o, low_o, nquad_o, nlow_o):
    prompt = pl.program_id(0)
    local = (prompt + 2 * s[0]) % 4
    keep = s[8 + prompt] == s[2]

    def write(wide, low, at):
        for f in range(4):
            for h in range(OWN):
                piece = wide[f, (at * OWN + h) * 64 : (at * OWN + h + 1) * 64].astype(F32)
                quad_o[0, 0, f * OWN + h] = jnp.where(keep, piece, 0.0)
                norm = wide[f, 512 + at * OWN + h : 513 + at * OWN + h].astype(F32)
                nquad_o[0, 0, f * OWN + h : f * OWN + h + 1] = jnp.where(keep, norm, 0.0)[:, :64]
        for h in range(OWN):
            piece = low[at * OWN + h].astype(F32)
            piece = jnp.where(keep, piece, 0.0)
            low_o[0, 0, h] = piece[: FD + 1]
            at_norm = NORM + 1 - LOW
            nlow_o[0, 0, h : h + 1] = piece[at_norm : at_norm + 1, : FD + 1]

    for at in range(2):

        @pl.when(local == at)
        def _():
            write(mine, low_mine, at)

        @pl.when(local == 2 + at)
        def _():
            write(theirs, low_theirs, at)


def grid_call(kernel, grid, in_specs, out_specs, out_shape, scratch=(), flops=0, scalars=1):
    return pl.pallas_call(
        kernel,
        grid_spec=pltpu.PrefetchScalarGridSpec(
            num_scalar_prefetch=scalars, grid=grid, in_specs=in_specs, out_specs=out_specs, scratch_shapes=scratch
        ),
        out_shape=out_shape,
        cost_estimate=pl.CostEstimate(flops=flops, transcendentals=0, bytes_accessed=1 << 20),
        compiler_params=pltpu.CompilerParams(dimension_semantics=("arbitrary",) * len(grid)),
    )


def shape(dims, dtype=BF):
    return jax.ShapeDtypeStruct(dims, dtype)


def whole(*dims):
    return pl.BlockSpec(dims, lambda i, *_: (0,) * len(dims))


def per_step(*dims):
    return pl.BlockSpec((1,) + dims, lambda i, *_: (i,) + (0,) * len(dims))


def body(hidden_in, w_query, w_key, w_value, lengths, owners):
    core = lax.axis_index("c")
    feat = lax.axis_index("feat")
    chip = lax.axis_index("z") * 4 + lax.axis_index("y")
    seq = chip * 2 + core
    local = (jnp.arange(4) + 2 * core) % 4
    slice_prompt = 2 * core + chip // 16
    s = jnp.concatenate(
        [
            jnp.stack([core, feat % 2, seq]).astype(jnp.int32),
            lengths[local],
            (owners[slice_prompt] // 2)[None],
            owners,
            (feat // 2)[None].astype(jnp.int32),
        ]
    )
    picks = jnp.asarray(PICKS, BF)
    spread = jnp.asarray(SPREAD, BF)
    swap = [(0, 1), (1, 0)]

    picks_spec = pl.BlockSpec((1, 2, OWN * ROWS, 128), lambda i, s: (s[1], 0, 0, 0))
    q, k, v, send, keep = grid_call(
        project_kernel,
        (4,),
        [
            pl.BlockSpec((1, SPAN, D), lambda i, s: ((i + 2 + 2 * s[0]) % 4, 0, 0)),
            whole(D, 512),
            pl.BlockSpec((D, 128), lambda i, s: (0, s[12])),
            pl.BlockSpec((D, 128), lambda i, s: (0, s[12])),
            picks_spec,
        ],
        [
            pl.BlockSpec((1, SPAN, 128), lambda i, s: ((i + 2) % 4, 0, 0)),
            pl.BlockSpec((1, SPAN, 128), lambda i, s: ((i + 2) % 4, 0, 0)),
            pl.BlockSpec((1, SPAN, 512), lambda i, s: ((i + 2) % 4, 0, 0)),
            pl.BlockSpec((1, OWN * ROWS, HD), lambda i, s: (jnp.minimum(i, 1), 0, 0)),
            pl.BlockSpec((1, OWN * ROWS, HD), lambda i, s: (jnp.maximum(i - 2, 0), 0, 0)),
        ],
        [
            shape((4, SPAN, 128)),
            shape((4, SPAN, 128)),
            shape((4, SPAN, 512)),
            shape((2, OWN * ROWS, HD)),
            shape((2, OWN * ROWS, HD)),
        ],
        [pltpu.VMEM((D, 256), BF)],
        flops=3_000_000_000,
    )(s, hidden_in, w_value, w_query, w_key, picks)

    recv = lax.ppermute(send, "c", swap)
    pair = (keep.astype(F32) + recv.astype(F32)).astype(BF).reshape(CHIPS, SLICE, HD)
    pieces = lax.all_to_all(pair, CHIP, 0, 0)

    num, den, feats = grid_call(
        self_kernel,
        (4,),
        [per_step(SPAN, 128), per_step(SPAN, 128), per_step(SPAN, 512), picks_spec, whole(8, ROWS)],
        [per_step(SPAN, 512), per_step(SPAN, 128), per_step(OWN, SPAN, ROWS)],
        [shape((4, SPAN, 512), F32), shape((4, SPAN, 128), F32), shape((4, OWN, SPAN, ROWS))],
        flops=2_000_000_000,
    )(s, q, k, v, picks, jnp.asarray(LINES))

    both = grid_call(
        scan_kernel,
        (1,),
        [whole(CHIPS, SLICE, HD)],
        whole(CHIPS, 2 * SLICE, HD),
        shape((CHIPS, 2 * SLICE, HD)),
    )(s, pieces)
    back = lax.all_to_all(both, CHIP, 0, 0)
    back_spec = [pl.BlockSpec((CHIPS, SLICE, HD), functools.partial(lambda n, i, *_: (0, n, 0), n)) for n in range(2)]
    half = whole(2, OWN * ROWS, HD)
    own_state, their_state = grid_call(
        prefix_kernel,
        (1,),
        [back_spec[0], half, half],
        [half, half],
        [shape((2, OWN * ROWS, HD)), shape((2, OWN * ROWS, HD))],
    )(s, back, keep, recv)
    other_state = lax.ppermute(their_state, "c", swap)

    wide, low = grid_call(
        spread_kernel,
        (1,),
        [back_spec[1], whole(FD * FD, ROWS)],
        [whole(4, 520, HD), whole(2 * OWN, ROWS - LOW, HD)],
        [shape((4, 520, HD)), shape((2 * OWN, ROWS - LOW, HD))],
        scalars=0,
    )(back, spread)
    wide = lax.all_to_all(wide, "feat", 0, 0)

    def attend(state, first):
        shifted = lambda *dims: pl.BlockSpec((1,) + dims, lambda i, *_: (i + first,) + (0,) * len(dims))
        return grid_call(
            lambda s, *refs: attend_kernel(s, first, *refs),
            (2,),
            [per_step(OWN * ROWS, HD), shifted(SPAN, 512), shifted(SPAN, 128), shifted(OWN, SPAN, ROWS)],
            [per_step(SPAN, 512), per_step(8, SPAN)],
            [shape((2, SPAN, 512), F32), shape((2, 8, SPAN), F32)],
            flops=500_000_000,
        )(s, state, num, den, feats)

    own_att, own_square = attend(own_state, 0)
    other_att, other_square = attend(other_state, 2)
    square = jnp.concatenate([own_square[:, :1], other_square[:, :1]], axis=0)
    square = square + lax.ppermute(square, "feat", [(n, n ^ 1) for n in range(4)])
    square = square + lax.ppermute(square, "feat", [(n, 3 - n) for n in range(4)])
    mixed = grid_call(
        mix_kernel,
        (4,),
        [
            pl.BlockSpec((1, SPAN, 512), lambda i, s: (jnp.minimum(i, 1), 0, 0)),
            pl.BlockSpec((1, SPAN, 512), lambda i, s: (jnp.maximum(i - 2, 0), 0, 0)),
            per_step(1, SPAN),
        ],
        pl.BlockSpec((1, SPAN, 512), lambda i, s: ((i + 2 * s[0]) % 4, 0, 0)),
        shape((4, SPAN, 512)),
    )(s, own_att, other_att, square)

    their_wide = lax.ppermute(wide, "c", swap)
    their_low = lax.ppermute(low, "c", swap)
    quad, low_out, norm_quad, norm_low = grid_call(
        final_kernel,
        (4,),
        [
            whole(4, 520, HD),
            whole(4, 520, HD),
            whole(2 * OWN, ROWS - LOW, HD),
            whole(2 * OWN, ROWS - LOW, HD),
        ],
        [
            pl.BlockSpec((1, 1, H, 64, HD), lambda i, s: (0, i, 0, 0, 0)),
            pl.BlockSpec((1, 1, OWN, FD + 1, HD), lambda i, s: (0, i, 0, 0, 0)),
            pl.BlockSpec((1, 1, H, 64), lambda i, s: (0, i, 0, 0)),
            pl.BlockSpec((1, 1, OWN, FD + 1), lambda i, s: (0, i, 0, 0)),
        ],
        [
            shape((1, 4, H, 64, HD), F32),
            shape((1, 4, OWN, FD + 1, HD), F32),
            shape((1, 4, H, 64), F32),
            shape((1, 4, OWN, FD + 1), F32),
        ],
    )(s, wide, their_wide, low, their_low)
    return mixed, quad, low_out, norm_quad, norm_low


def solution(mesh):
    torus = Mesh(mesh.devices.reshape(8, 4, 2, 4), ("z", "y", "c", "feat"))
    seq = ("z", "y", "c")
    return jax.shard_map(
        body,
        mesh=torus,
        in_specs=(P(None, seq, None), P(), P(), P(None, "feat"), P(), P()),
        out_specs=(
            P(None, seq, "feat"),
            P(seq, None, None, "feat", None),
            P(seq, None, "feat", None, None),
            P(seq, None, None, "feat"),
            P(seq, None, "feat", None),
        ),
        check_vma=False,
    )
```

```python
import functools

import jax
import jax.numpy as jnp
import numpy as np
from jax import lax
from jax.experimental import pallas as pl
from jax.experimental.pallas import tpu as pltpu
from jax.sharding import Mesh
from jax.sharding import PartitionSpec as P

H = 16
FD = 16
HD = 128
D = 2048
SPAN = 256
OWN = 4
ROWS = 160
QUADS = 136
LOW = 128
NORM = 153
CHIPS = 32
SLICE = 2 * OWN * ROWS // CHIPS
NORM_FLOOR = 0.0001
BF = jnp.bfloat16
F32 = jnp.float32
CHIP = ("z", "y")


def feature_rows():
    pairs = [(i, j) for i in range(FD) for j in range(i, FD)]
    rows = [u if u < LOW else u + FD + 1 for u in range(QUADS)]
    return pairs, rows


def tables():
    pairs, rows = feature_rows()
    first = np.zeros((ROWS, FD), np.float32)
    second = np.zeros((ROWS, FD), np.float32)
    spread = np.zeros((FD * FD, ROWS), np.float32)
    for (i, j), row in zip(pairs, rows):
        first[row, i] = 1
        second[row, j] = 1
        spread[i * FD + j, row] = 1
        spread[j * FD + i, row] = 1
    for i in range(FD):
        first[LOW + 1 + i, i] = 1
    picks = np.zeros((2, 2, OWN, ROWS, 2 * OWN * FD), np.float32)
    for half in range(2):
        for head in range(OWN):
            at = half * OWN * FD + head * FD
            picks[half, 0, head, :, at : at + FD] = first
            picks[half, 1, head, :, at : at + FD] = second
    lines = np.zeros((8, ROWS), np.float32)
    for (i, j), row in zip(pairs, rows):
        lines[0, row] = (1.0 if i == j else 2.0) * (2.0 * FD) ** -0.5
    lines[0, LOW + 1 : LOW + 1 + FD] = lines[1, LOW + 1 : LOW + 1 + FD] = FD**-0.25
    lines[:3, LOW] = 1.0
    return picks.reshape(2, 2, OWN * ROWS, 2 * OWN * FD), spread, lines


PICKS, SPREAD, LINES = tables()


def is_low(row):
    return (row >= LOW) & (row <= LOW + FD)


def nt(a, b):
    return lax.dot_general(a, b, (((1,), (1,)), ((), ())), preferred_element_type=F32)


def place():
    core = lax.axis_index("c")
    chip = lax.axis_index("z") * 4 + lax.axis_index("y")
    return core, chip, chip * 2 + core, lax.axis_index("feat")


CHUNK = 512


def project_kernel(
    lens_h, hid, wv, wq, wk, picks_h, q_o, k_o, v_o, send_o, keep_o, picks, hid_b, wv_b, wqk_b, lens, sems, rest, small
):
    core, _, seq, feat = place()
    lanes = pl.ds(pl.multiple_of(feat // 2 * 128, 128), 128)
    first = (2 + 2 * core) % 4
    early = []
    for n in range(D // CHUNK):
        rows = pl.ds(n * CHUNK, CHUNK)
        early.append(
            [
                pltpu.make_async_copy(hid.at[first, :, rows], hid_b.at[2, :, rows], sems.at[n, 0]),
                pltpu.make_async_copy(wq.at[rows, lanes], wqk_b.at[rows, :128], sems.at[n, 1]),
                pltpu.make_async_copy(wk.at[rows, lanes], wqk_b.at[rows, 128:], sems.at[n, 2]),
                pltpu.make_async_copy(wv.at[rows], wv_b.at[rows], sems.at[n, 3]),
            ]
        )
        for copy in early[-1]:
            copy.start()
    tiny = [
        pltpu.make_async_copy(lens_h, lens, small.at[0]),
        pltpu.make_async_copy(picks_h.at[feat % 2], picks, small.at[1]),
    ]
    for copy in tiny:
        copy.start()
    late = []
    for n, local in enumerate((3, 0, 1)):
        late.append(pltpu.make_async_copy(hid.at[(local + 2 * core) % 4], hid_b.at[local], rest.at[n]))
        late[-1].start()
    row = lax.broadcasted_iota(jnp.int32, (ROWS, SPAN), 0)
    low = is_low(row)
    const = (row == LOW).astype(F32)
    fixed = jnp.where(row == LOW, 1.0, jnp.where(low, FD**-0.25, (2.0 * FD) ** -0.5))
    ones = jnp.ones((8, SPAN), BF)
    tail_row = lax.broadcasted_iota(jnp.int32, (8, HD), 0) + (ROWS - 8)
    for n, local in enumerate((2, 3, 0, 1)):
        if n == 0:
            v = jnp.zeros((SPAN, 512), F32)
            qk = jnp.zeros((SPAN, 256), F32)
            for m in range(D // CHUNK):
                for copy in early[m]:
                    copy.wait()
                rows = slice(m * CHUNK, (m + 1) * CHUNK)
                x = hid_b[local, :, rows]
                qk = qk + jnp.dot(x, wqk_b[rows], preferred_element_type=F32)
                v = v + jnp.dot(x, wv_b[rows], preferred_element_type=F32)
            for copy in tiny:
                copy.wait()
        else:
            late[n - 1].wait()
            x = hid_b[local]
            qk = jnp.dot(x, wqk_b[...], preferred_element_type=F32)
            v = jnp.dot(x, wv_b[...], preferred_element_type=F32)
        v = v.astype(BF)
        key = qk[:, 128:].astype(BF)
        q_o[local] = qk[:, :128].astype(BF)
        v_o[local] = v
        k_o[local] = key
        key_t = key.astype(F32).T.astype(BF)
        token = seq * SPAN + lax.broadcasted_iota(jnp.int32, (1, SPAN), 1)
        scale = jnp.where(token < lens[(local + 2 * core) % 4], fixed, 0.0)
        bias = jnp.where(low, scale, 0.0)
        target = send_o if local >= 2 else keep_o
        for h in range(OWN):
            at = h * ROWS
            u = jnp.dot(picks[0, at : at + ROWS], key_t, preferred_element_type=F32)
            w = jnp.dot(picks[1, at : at + ROWS], key_t, preferred_element_type=F32)
            feats = ((u + const) * (w * scale + bias)).astype(BF)
            state = jnp.dot(feats, v[:, h * HD : (h + 1) * HD], preferred_element_type=F32)
            norm = nt(ones, feats)
            rest_norm = jnp.concatenate([norm[:, HD:], jnp.zeros((8, 2 * HD - ROWS), F32)], axis=1)
            tail = state[ROWS - 8 :]
            tail = jnp.where(tail_row == NORM, norm[:, :HD], jnp.where(tail_row == NORM + 1, rest_norm, tail))
            target[local % 2, at : at + ROWS] = jnp.concatenate([state[: ROWS - 8], tail], axis=0).astype(BF)


def self_kernel(lens, q, k, v, picks, lines, num_o, den_o, feat_o):
    core, _, seq, feat = place()
    tq = lax.broadcasted_iota(jnp.int32, (SPAN, SPAN), 0)
    tk = lax.broadcasted_iota(jnp.int32, (SPAN, SPAN), 1)
    lane = lax.broadcasted_iota(jnp.int32, (SPAN, HD), 1)
    scale, bias, const = lines[0:1], lines[1:2], lines[2:3]
    ones = jnp.ones((SPAN, HD), BF)

    def prompt(local, _):
        query = q[local]
        key = k[local]
        seen = (tk <= tq) & (seq * SPAN + tk < lens[(local + 2 * core) % 4])
        den_all = jnp.zeros((SPAN, HD), F32)
        for h in range(OWN):
            at = h * ROWS
            mine = jnp.where(lane // FD == feat % 2 * OWN + h, query, jnp.zeros_like(query))
            score = nt(mine, key)
            weight = jnp.where(seen, 1.0 + score * (FD**-0.5) + score * score * (0.5 / FD), 0.0).astype(BF)
            value = v[local, :, h * HD : (h + 1) * HD]
            num_o[local, :, h * HD : (h + 1) * HD] = jnp.dot(weight, value, preferred_element_type=F32)
            den = jnp.dot(weight, ones, preferred_element_type=F32)
            den_all = jnp.where(lane == h, den, den_all)
            u = nt(query, picks[0, at : at + ROWS])
            w = nt(query, picks[1, at : at + ROWS])
            feat_o[local, h] = ((u + const) * (w * scale + bias)).astype(BF)
        den_o[local] = den_all
        return _

    lax.fori_loop(0, 4, prompt, 0)


def pair_kernel(keep, recv, after, out):
    pair = (keep[...].astype(F32) + recv[...].astype(F32)).astype(BF)
    out[...] = pair.reshape(CHIPS, SLICE, HD)


def scan_kernel(owners, pieces, out):
    core, chip, _, _ = place()
    home = owners[2 * core + chip // 16] // 2
    before = jnp.zeros((SLICE, HD), F32)
    for n in range(CHIPS):
        out[n, :SLICE] = before.astype(BF)
        before = before + pieces[n].astype(F32)
    total = before.astype(BF)
    nothing = jnp.zeros_like(total)
    for n in range(CHIPS):
        out[n, SLICE:] = jnp.where(home == n, total, nothing)


STATE = 2 * OWN * ROWS
LOW_ROWS = ROWS - LOW
WIDE = 2 * OWN * 64
NORMS = WIDE + 8
SENT = NORMS + 16


def prefix_kernel(back, keep, recv, own_o, other_o):
    before = back[:, :SLICE].reshape(STATE, HD).astype(F32)
    second = lax.axis_index("c") == 1
    added = jnp.where(second, recv[...], keep[...]).reshape(STATE, HD).astype(F32)
    both = (before + added).astype(BF)
    plain = before.astype(BF)
    own_o[...] = jnp.where(second, both, plain).reshape(2, OWN * ROWS, HD)
    other_o[:STATE] = jnp.where(second, plain, both)
    total = back[:, SLICE:].reshape(2 * OWN, ROWS, HD)
    other_o[STATE:] = total[:, LOW:].reshape(2 * OWN * LOW_ROWS, HD)


def norm_row(part):
    return jnp.concatenate([part[NORM : NORM + 1], part[NORM + 1 : NORM + 2, : ROWS - HD]], axis=1)


def spread(total, table, out):
    for n in range(2 * OWN):
        wide = jnp.dot(table[...], total[n], preferred_element_type=F32).astype(BF)
        for f in range(4):
            out[f, n * 64 : (n + 1) * 64] = wide[f * 64 : (f + 1) * 64]
    norm = nt(jnp.concatenate([norm_row(total[n]) for n in range(2 * OWN)], axis=0), table[...])
    pad = jnp.zeros((8, 64), F32)
    for f in range(4):
        out[f, WIDE:NORMS] = jnp.concatenate([norm[:, f * 64 : (f + 1) * 64], pad], axis=1).astype(BF)


def attend(first, lens, state, num, den, feat, att_o):
    core, _, seq, _ = place()
    token = seq * SPAN + lax.broadcasted_iota(jnp.int32, (SPAN, HD), 0)
    ones = jnp.ones((8, HD), F32)
    found = []
    for n in range(2):
        live = token < lens[(first + n + 2 * core) % 4]
        den_all = den[first + n]
        squares = jnp.zeros((SPAN, HD), F32)
        for h in range(OWN):
            feats = feat[first + n, h]
            part = state(n, h)
            total = num[first + n, :, h * HD : (h + 1) * HD] + jnp.dot(feats, part, preferred_element_type=F32)
            below = nt(feats, jnp.broadcast_to(norm_row(part), (HD, ROWS))) + den_all[:, h : h + 1]
            att = jnp.where(live, total / below, 0.0)
            att_o[n, :, h * HD : (h + 1) * HD] = att
            squares = squares + att * att
        sums = lax.dot_general(
            ones,
            squares,
            (((1,), (1,)), ((), ())),
            precision=lax.Precision.HIGHEST,
            preferred_element_type=F32,
        )
        found += [sums[:1, :HD], sums[:1, HD:]]
    return found


def own_kernel(lens, state, num, den, feat, att_o, square_o):
    found = attend(0, lens, lambda n, h: state[n, h * ROWS : (h + 1) * ROWS], num, den, feat, att_o)
    square_o[...] = jnp.concatenate(found + [jnp.zeros((4, HD), F32)], axis=0)


def other_kernel(lens, state, num, den, feat, square, back, table, att_o, sent_o):
    def part(n, h):
        at = (n * OWN + h) * ROWS
        return state[at : at + ROWS]

    found = attend(2, lens, part, num, den, feat, att_o)
    squares = jnp.concatenate([square[:4]] + found, axis=0)
    high = squares.astype(BF)
    rest = (squares - high.astype(F32)).astype(BF)
    for f in range(4):
        sent_o[f, NORMS : NORMS + 8] = high
        sent_o[f, NORMS + 8 :] = rest
    spread(back[:, SLICE:].reshape(2 * OWN, ROWS, HD), table, sent_o)


def mix_kernel(own, other, sent, mixed_o):
    step = pl.program_id(0)
    square = jnp.zeros((8, HD), F32)
    for f in range(4):
        square = square + (sent[f, NORMS : NORMS + 8].astype(F32) + sent[f, NORMS + 8 :].astype(F32))
    factor = lax.rsqrt(square * (1.0 / D) + NORM_FLOOR).T
    lane = lax.broadcasted_iota(jnp.int32, (HD, 8), 1)
    for k in range(2):
        column = jnp.sum(jnp.where(lane == 2 * step + k, factor, 0.0), axis=1, keepdims=True)
        rows = slice(k * HD, (k + 1) * HD)

        @pl.when(step < 2)
        def _():
            mixed_o[0, rows] = (own[step, rows] * column).astype(BF)

        @pl.when(step >= 2)
        def _():
            mixed_o[0, rows] = (other[step - 2, rows] * column).astype(BF)


def final_kernel(owners, mine, theirs, low_mine, low_theirs, quad_o, low_o, nquad_o, nlow_o):
    core, _, seq, _ = place()
    prompt = pl.program_id(0)
    local = (prompt + 2 * core) % 4
    keep = owners[prompt] == seq

    def write(wide, low, at):
        for f in range(4):
            for h in range(OWN):
                piece = wide[f, (at * OWN + h) * 64 : (at * OWN + h + 1) * 64].astype(F32)
                quad_o[0, 0, f * OWN + h] = jnp.where(keep, piece, 0.0)
                norm = wide[f, WIDE + at * OWN + h : WIDE + 1 + at * OWN + h].astype(F32)
                nquad_o[0, 0, f * OWN + h : f * OWN + h + 1] = jnp.where(keep, norm, 0.0)[:, :64]
        for h in range(OWN):
            piece = low[pl.ds(STATE + (at * OWN + h) * LOW_ROWS, LOW_ROWS)].astype(F32)
            piece = jnp.where(keep, piece, 0.0)
            for r in range(FD + 1):
                low_o[0, 0, r, h : h + 1] = piece[r : r + 1]
            at_norm = NORM + 1 - LOW
            nlow_o[0, 0, h : h + 1] = piece[at_norm : at_norm + 1, : FD + 1]

    for at in range(2):

        @pl.when(local == at)
        def _():
            write(mine, low_mine, at)

        @pl.when(local == 2 + at)
        def _():
            write(theirs, low_theirs, at)


SMEM = pl.BlockSpec(memory_space=pltpu.SMEM)
VMEM = pl.BlockSpec(memory_space=pltpu.VMEM)
ANY = pl.BlockSpec(memory_space=pl.ANY)
MIB = 1 << 20


def near(*arrays):
    return [pltpu.with_memory_space_constraint(a, pltpu.VMEM) for a in arrays]


def call(kernel, in_specs, out_shape, out_specs=None, grid=(), scratch=(), flops=0, limit=16):
    if out_specs is None:
        out_specs = jax.tree.map(lambda _: VMEM, out_shape, is_leaf=lambda x: not isinstance(x, (list, tuple)))
    return pl.pallas_call(
        kernel,
        grid=grid,
        in_specs=in_specs,
        out_specs=out_specs,
        out_shape=out_shape,
        scratch_shapes=scratch,
        cost_estimate=pl.CostEstimate(flops=flops, transcendentals=0, bytes_accessed=MIB),
        compiler_params=pltpu.CompilerParams(
            dimension_semantics=("arbitrary",) * len(grid), vmem_limit_bytes=limit * MIB
        ),
    )


def far(dims, dtype=BF):
    return jax.ShapeDtypeStruct(dims, dtype)


def shape(dims, dtype=BF):
    return pltpu.VMEM(dims, dtype)


def held(*arrays):
    return [pltpu.with_memory_space_constraint(a, pltpu.HBM) for a in arrays]


def body(hidden_in, w_query, w_key, w_value, lengths, owners):
    swap = [(0, 1), (1, 0)]
    half = (2, OWN * ROWS, HD)
    packed = OWN * ROWS

    q, k, v, send, keep, picks = call(
        project_kernel,
        [ANY] * 6,
        [
            shape((4, SPAN, 128)),
            shape((4, SPAN, 128)),
            shape((4, SPAN, 512)),
            shape(half),
            shape(half),
            shape((2, packed, 128)),
        ],
        scratch=[
            pltpu.VMEM((4, SPAN, D), BF),
            pltpu.VMEM((D, 512), BF),
            pltpu.VMEM((D, 256), BF),
            pltpu.SMEM((4,), jnp.int32),
            pltpu.SemaphoreType.DMA((D // CHUNK, 4)),
            pltpu.SemaphoreType.DMA((3,)),
            pltpu.SemaphoreType.DMA((2,)),
        ],
        flops=3_000_000_000,
        limit=24,
    )(*held(lengths, hidden_in, w_value, w_query, w_key, jnp.asarray(PICKS, BF)))

    recv = lax.ppermute(send, "c", swap)
    num, den, feats = call(
        self_kernel,
        [SMEM] + [VMEM] * 5,
        [shape((4, SPAN, 512), F32), shape((4, SPAN, 128), F32), shape((4, OWN, SPAN, ROWS))],
        flops=3_000_000_000,
    )(lengths, *near(q, k, v, picks, jnp.asarray(LINES)))
    pair = call(pair_kernel, [VMEM, VMEM, ANY], shape((CHIPS, SLICE, HD)))(*near(keep, recv, den))
    pieces = lax.all_to_all(pair, CHIP, 0, 0)
    both = call(scan_kernel, [SMEM, VMEM], shape((CHIPS, 2 * SLICE, HD)))(owners, *near(pieces))
    back = lax.all_to_all(both, CHIP, 0, 0)
    own_state, given = call(
        prefix_kernel, [VMEM] * 3, [shape(half), shape((STATE + 2 * OWN * LOW_ROWS, HD))]
    )(*near(back, keep, recv))
    taken = lax.ppermute(given, "c", swap)

    own_att, square = call(
        own_kernel,
        [SMEM] + [VMEM] * 4,
        [shape((2, SPAN, 512), F32), shape((8, HD), F32)],
        flops=500_000_000,
    )(lengths, *near(own_state, num, den, feats))
    other_att, sent = call(
        other_kernel,
        [SMEM] + [VMEM] * 7,
        [shape((2, SPAN, 512), F32), shape((4, SENT, HD))],
        flops=500_000_000,
    )(lengths, *near(taken, num, den, feats, square, back, jnp.asarray(SPREAD, BF)))
    mine = lax.all_to_all(sent, "feat", 0, 0)
    theirs = lax.ppermute(mine, "c", swap)
    mixed = call(
        mix_kernel,
        [VMEM] * 3,
        far((4, SPAN, 512)),
        pl.BlockSpec((1, SPAN, 512), lambda i: ((i + 2 * lax.axis_index("c")) % 4, 0, 0)),
        (4,),
        flops=500_000_000,
    )(*near(own_att, other_att, mine))

    quad, low_out, norm_quad, norm_low = call(
        final_kernel,
        [SMEM] + [VMEM] * 4,
        [
            far((1, 4, H, 64, HD), F32),
            far((1, 4, FD + 1, OWN, HD), F32),
            far((1, 4, H, 64), F32),
            far((1, 4, OWN, FD + 1), F32),
        ],
        [
            pl.BlockSpec((1, 1, H, 64, HD), lambda i: (0, i, 0, 0, 0)),
            pl.BlockSpec((1, 1, FD + 1, OWN, HD), lambda i: (0, i, 0, 0, 0)),
            pl.BlockSpec((1, 1, H, 64), lambda i: (0, i, 0, 0)),
            pl.BlockSpec((1, 1, OWN, FD + 1), lambda i: (0, i, 0, 0)),
        ],
        (4,),
    )(owners, *near(mine, theirs, given, taken))
    return mixed, quad, jnp.transpose(low_out, (0, 1, 3, 2, 4)), norm_quad, norm_low


def solution(mesh):
    torus = Mesh(mesh.devices.reshape(8, 4, 2, 4), ("z", "y", "c", "feat"))
    seq = ("z", "y", "c")
    return jax.shard_map(
        body,
        mesh=torus,
        in_specs=(P(None, seq, None), P(), P(), P(None, "feat"), P(), P()),
        out_specs=(
            P(None, seq, "feat"),
            P(seq, None, None, "feat", None),
            P(seq, None, "feat", None, None),
            P(seq, None, None, "feat"),
            P(seq, None, "feat", None),
        ),
        check_vma=False,
    )
```

```python
import functools

import jax
import jax.numpy as jnp
import numpy as np
from jax import lax
from jax.experimental import pallas as pl
from jax.experimental.pallas import tpu as pltpu
from jax.sharding import Mesh
from jax.sharding import PartitionSpec as P

H = 16
FD = 16
HD = 128
D = 2048
SPAN = 256
OWN = 4
ROWS = 160
QUADS = 136
LOW = 128
NORM = 153
CHIPS = 32
SLICE = 2 * OWN * ROWS // CHIPS
NORM_FLOOR = 0.0001
BF = jnp.bfloat16
F32 = jnp.float32
CHIP = ("z", "y")


def feature_rows():
    pairs = [(i, j) for i in range(FD) for j in range(i, FD)]
    rows = [u if u < LOW else u + FD + 1 for u in range(QUADS)]
    return pairs, rows


def tables():
    pairs, rows = feature_rows()
    first = np.zeros((ROWS, FD), np.float32)
    second = np.zeros((ROWS, FD), np.float32)
    spread = np.zeros((FD * FD, ROWS), np.float32)
    for (i, j), row in zip(pairs, rows):
        first[row, i] = 1
        second[row, j] = 1
        spread[i * FD + j, row] = 1
        spread[j * FD + i, row] = 1
    for i in range(FD):
        first[LOW + 1 + i, i] = 1
    picks = np.zeros((2, 2, OWN, ROWS, 2 * OWN * FD), np.float32)
    for half in range(2):
        for head in range(OWN):
            at = half * OWN * FD + head * FD
            picks[half, 0, head, :, at : at + FD] = first
            picks[half, 1, head, :, at : at + FD] = second
    lines = np.zeros((8, ROWS), np.float32)
    for (i, j), row in zip(pairs, rows):
        lines[0, row] = (1.0 if i == j else 2.0) * (2.0 * FD) ** -0.5
    lines[0, LOW + 1 : LOW + 1 + FD] = lines[1, LOW + 1 : LOW + 1 + FD] = FD**-0.25
    lines[:3, LOW] = 1.0
    return picks.reshape(2, 2, OWN * ROWS, 2 * OWN * FD), spread, lines


PICKS, SPREAD, LINES = tables()


def is_low(row):
    return (row >= LOW) & (row <= LOW + FD)


def nt(a, b):
    return lax.dot_general(a, b, (((1,), (1,)), ((), ())), preferred_element_type=F32)


def place():
    core = lax.axis_index("c")
    chip = lax.axis_index("z") * 4 + lax.axis_index("y")
    return core, chip, chip * 2 + core, lax.axis_index("feat")


CHUNK = 512
AHEAD = 5


def project_kernel(
    lens_h, hid, wv, wq, wk, picks_h, q_o, k_o, v_o, send_o, keep_o, picks, hid_b, wv_b, wqk_b, lens, sems, rest, small
):
    core, _, seq, feat = place()
    lanes = pl.ds(pl.multiple_of(feat // 2 * 128, 128), 128)
    first = (2 + 2 * core) % 4
    queue = []
    for n in range(D // CHUNK):
        rows = pl.ds(n * CHUNK, CHUNK)
        queue.append(
            [
                pltpu.make_async_copy(hid.at[first, :, rows], hid_b.at[2, :, rows], sems.at[n, 0]),
                pltpu.make_async_copy(wq.at[rows, lanes], wqk_b.at[rows, :128], sems.at[n, 1]),
                pltpu.make_async_copy(wk.at[rows, lanes], wqk_b.at[rows, 128:], sems.at[n, 2]),
                pltpu.make_async_copy(wv.at[rows], wv_b.at[rows], sems.at[n, 3]),
            ]
        )
    queue.append(
        [
            pltpu.make_async_copy(lens_h, lens, small.at[0]),
            pltpu.make_async_copy(picks_h.at[feat % 2], picks, small.at[1]),
        ]
    )
    for n, local in enumerate((3, 0, 1)):
        queue.append([pltpu.make_async_copy(hid.at[(local + 2 * core) % 4], hid_b.at[local], rest.at[n])])

    def start(n):
        if n < len(queue):
            for copy in queue[n]:
                copy.start()

    def arrive(n):
        for copy in queue[n]:
            copy.wait()
        start(n + AHEAD)

    for n in range(AHEAD):
        start(n)
    row = lax.broadcasted_iota(jnp.int32, (ROWS, SPAN), 0)
    low = is_low(row)
    const = (row == LOW).astype(F32)
    fixed = jnp.where(row == LOW, 1.0, jnp.where(low, FD**-0.25, (2.0 * FD) ** -0.5))
    ones = jnp.ones((8, SPAN), BF)
    tail_row = lax.broadcasted_iota(jnp.int32, (8, HD), 0) + (ROWS - 8)

    def project(n, local):
        if n == 0:
            v = jnp.zeros((SPAN, 512), F32)
            qk = jnp.zeros((SPAN, 256), F32)
            for m in range(D // CHUNK):
                arrive(m)
                rows = slice(m * CHUNK, (m + 1) * CHUNK)
                x = hid_b[local, :, rows]
                qk = qk + jnp.dot(x, wqk_b[rows], preferred_element_type=F32)
                v = v + jnp.dot(x, wv_b[rows], preferred_element_type=F32)
            arrive(D // CHUNK)
        else:
            arrive(D // CHUNK + n)
            x = hid_b[local]
            qk = jnp.dot(x, wqk_b[...], preferred_element_type=F32)
            v = jnp.dot(x, wv_b[...], preferred_element_type=F32)
        q_o[local] = qk[:, :128].astype(BF)
        k_o[local] = qk[:, 128:].astype(BF)
        v_o[local] = v.astype(BF)

    def states(local):
        key_t = k_o[local].astype(F32).T.astype(BF)
        token = seq * SPAN + lax.broadcasted_iota(jnp.int32, (1, SPAN), 1)
        scale = jnp.where(token < lens[(local + 2 * core) % 4], fixed, 0.0)
        bias = jnp.where(low, scale, 0.0)
        target = send_o if local >= 2 else keep_o
        for h in range(OWN):
            at = h * ROWS
            u = jnp.dot(picks[0, at : at + ROWS], key_t, preferred_element_type=F32)
            w = jnp.dot(picks[1, at : at + ROWS], key_t, preferred_element_type=F32)
            feats = ((u + const) * (w * scale + bias)).astype(BF)
            state = jnp.dot(feats, v_o[local, :, h * HD : (h + 1) * HD], preferred_element_type=F32)
            norm = nt(ones, feats)
            rest_norm = jnp.concatenate([norm[:, HD:], jnp.zeros((8, 2 * HD - ROWS), F32)], axis=1)
            tail = state[ROWS - 8 :]
            tail = jnp.where(tail_row == NORM, norm[:, :HD], jnp.where(tail_row == NORM + 1, rest_norm, tail))
            target[local % 2, at : at + ROWS] = jnp.concatenate([state[: ROWS - 8], tail], axis=0).astype(BF)

    order = (2, 3, 0, 1)
    for n in range(5):
        if n < 4:
            project(n, order[n])
        if n > 0:
            states(order[n - 1])


def self_kernel(lens, q, k, v, picks, lines, num_o, den_o, feat_o, late=False):
    core, _, seq, feat = place()
    split = jnp.maximum(4 - lax.axis_index("z"), 0)
    tq = lax.broadcasted_iota(jnp.int32, (SPAN, SPAN), 0)
    tk = lax.broadcasted_iota(jnp.int32, (SPAN, SPAN), 1)
    lane = lax.broadcasted_iota(jnp.int32, (SPAN, HD), 1)
    scale, bias, const = lines[0:1], lines[1:2], lines[2:3]
    ones = jnp.ones((SPAN, HD), BF)

    def prompt(local, _):
        query = q[local]
        key = k[local]
        seen = (tk <= tq) & (seq * SPAN + tk < lens[(local + 2 * core) % 4])
        den_all = jnp.zeros((SPAN, HD), F32)
        for h in range(OWN):
            at = h * ROWS
            mine = jnp.where(lane // FD == feat % 2 * OWN + h, query, jnp.zeros_like(query))
            score = nt(mine, key)
            weight = jnp.where(seen, 1.0 + score * (FD**-0.5) + score * score * (0.5 / FD), 0.0).astype(BF)
            value = v[local, :, h * HD : (h + 1) * HD]
            num_o[local, :, h * HD : (h + 1) * HD] = jnp.dot(weight, value, preferred_element_type=F32)
            den = jnp.dot(weight, ones, preferred_element_type=F32)
            den_all = jnp.where(lane == h, den, den_all)
            u = nt(query, picks[0, at : at + ROWS])
            w = nt(query, picks[1, at : at + ROWS])
            feat_o[local, h] = ((u + const) * (w * scale + bias)).astype(BF)
        den_o[local] = den_all
        return _

    lax.fori_loop(split if late else 0, 4 if late else split, prompt, 0)


def late_kernel(lens, q, k, v, picks, lines, num, den, feat, after, num_o, den_o, feat_o):
    self_kernel(lens, q, k, v, picks, lines, num_o, den_o, feat_o, late=True)


def pair_kernel(keep, recv, after, out):
    pair = (keep[...].astype(F32) + recv[...].astype(F32)).astype(BF)
    out[...] = pair.reshape(CHIPS, SLICE, HD)


def scan_kernel(owners, pieces, out):
    core, chip, _, _ = place()
    home = owners[2 * core + chip // 16] // 2
    before = jnp.zeros((SLICE, HD), F32)
    for n in range(CHIPS):
        out[n, :SLICE] = before.astype(BF)
        before = before + pieces[n].astype(F32)
    total = before.astype(BF)
    nothing = jnp.zeros_like(total)
    for n in range(CHIPS):
        out[n, SLICE:] = jnp.where(home == n, total, nothing)


STATE = 2 * OWN * ROWS
LOW_ROWS = ROWS - LOW
WIDE = 2 * OWN * 64
NORMS = WIDE + 8
SENT = NORMS + 16


def prefix_kernel(back, keep, recv, own_o, other_o):
    before = back[:, :SLICE].reshape(STATE, HD).astype(F32)
    second = lax.axis_index("c") == 1
    added = jnp.where(second, recv[...], keep[...]).reshape(STATE, HD).astype(F32)
    both = (before + added).astype(BF)
    plain = before.astype(BF)
    own_o[...] = jnp.where(second, both, plain).reshape(2, OWN * ROWS, HD)
    other_o[:STATE] = jnp.where(second, plain, both)
    total = back[:, SLICE:].reshape(2 * OWN, ROWS, HD)
    other_o[STATE:] = total[:, LOW:].reshape(2 * OWN * LOW_ROWS, HD)


def norm_row(part):
    return jnp.concatenate([part[NORM : NORM + 1], part[NORM + 1 : NORM + 2, : ROWS - HD]], axis=1)


def spread(total, table, out):
    for n in range(2 * OWN):
        wide = jnp.dot(table[...], total[n], preferred_element_type=F32).astype(BF)
        for f in range(4):
            out[f, n * 64 : (n + 1) * 64] = wide[f * 64 : (f + 1) * 64]
    norm = nt(jnp.concatenate([norm_row(total[n]) for n in range(2 * OWN)], axis=0), table[...])
    pad = jnp.zeros((8, 64), F32)
    for f in range(4):
        out[f, WIDE:NORMS] = jnp.concatenate([norm[:, f * 64 : (f + 1) * 64], pad], axis=1).astype(BF)


def attend(first, lens, state, num, den, feat, att_o):
    core, _, seq, _ = place()
    token = seq * SPAN + lax.broadcasted_iota(jnp.int32, (SPAN, HD), 0)
    ones = jnp.ones((8, HD), F32)
    found = []
    for n in range(2):
        live = token < lens[(first + n + 2 * core) % 4]
        den_all = den[first + n]
        squares = jnp.zeros((SPAN, HD), F32)
        for h in range(OWN):
            feats = feat[first + n, h]
            part = state(n, h)
            total = num[first + n, :, h * HD : (h + 1) * HD] + jnp.dot(feats, part, preferred_element_type=F32)
            below = nt(feats, jnp.broadcast_to(norm_row(part), (HD, ROWS))) + den_all[:, h : h + 1]
            att = jnp.where(live, total / below, 0.0)
            att_o[n, :, h * HD : (h + 1) * HD] = att
            squares = squares + att * att
        sums = lax.dot_general(
            ones,
            squares,
            (((1,), (1,)), ((), ())),
            precision=lax.Precision.HIGHEST,
            preferred_element_type=F32,
        )
        found += [sums[:1, :HD], sums[:1, HD:]]
    return found


def own_kernel(lens, state, num, den, feat, att_o, square_o):
    found = attend(0, lens, lambda n, h: state[n, h * ROWS : (h + 1) * ROWS], num, den, feat, att_o)
    square_o[...] = jnp.concatenate(found + [jnp.zeros((4, HD), F32)], axis=0)


def other_kernel(lens, state, num, den, feat, square, back, table, att_o, sent_o):
    def part(n, h):
        at = (n * OWN + h) * ROWS
        return state[at : at + ROWS]

    found = attend(2, lens, part, num, den, feat, att_o)
    squares = jnp.concatenate([square[:4]] + found, axis=0)
    high = squares.astype(BF)
    rest = (squares - high.astype(F32)).astype(BF)
    for f in range(4):
        sent_o[f, NORMS : NORMS + 8] = high
        sent_o[f, NORMS + 8 :] = rest
    spread(back[:, SLICE:].reshape(2 * OWN, ROWS, HD), table, sent_o)


def mix_kernel(own, other, sent, mixed_o):
    step = pl.program_id(0)
    square = jnp.zeros((8, HD), F32)
    for f in range(4):
        square = square + (sent[f, NORMS : NORMS + 8].astype(F32) + sent[f, NORMS + 8 :].astype(F32))
    factor = lax.rsqrt(square * (1.0 / D) + NORM_FLOOR).T
    lane = lax.broadcasted_iota(jnp.int32, (HD, 8), 1)
    for k in range(2):
        column = jnp.sum(jnp.where(lane == 2 * step + k, factor, 0.0), axis=1, keepdims=True)
        rows = slice(k * HD, (k + 1) * HD)

        @pl.when(step < 2)
        def _():
            mixed_o[0, rows] = (own[step, rows] * column).astype(BF)

        @pl.when(step >= 2)
        def _():
            mixed_o[0, rows] = (other[step - 2, rows] * column).astype(BF)


def final_kernel(owners, mine, theirs, low_mine, low_theirs, quad_o, low_o, nquad_o, nlow_o):
    core, _, seq, _ = place()
    prompt = pl.program_id(0)
    local = (prompt + 2 * core) % 4
    keep = owners[prompt] == seq

    def write(wide, low, at):
        for f in range(4):
            for h in range(OWN):
                piece = wide[f, (at * OWN + h) * 64 : (at * OWN + h + 1) * 64].astype(F32)
                quad_o[0, 0, f * OWN + h] = jnp.where(keep, piece, 0.0)
                norm = wide[f, WIDE + at * OWN + h : WIDE + 1 + at * OWN + h].astype(F32)
                nquad_o[0, 0, f * OWN + h : f * OWN + h + 1] = jnp.where(keep, norm, 0.0)[:, :64]
        for h in range(OWN):
            piece = low[pl.ds(STATE + (at * OWN + h) * LOW_ROWS, LOW_ROWS)].astype(F32)
            piece = jnp.where(keep, piece, 0.0)
            for r in range(FD + 1):
                low_o[0, 0, r, h : h + 1] = piece[r : r + 1]
            at_norm = NORM + 1 - LOW
            nlow_o[0, 0, h : h + 1] = piece[at_norm : at_norm + 1, : FD + 1]

    for at in range(2):

        @pl.when(local == at)
        def _():
            write(mine, low_mine, at)

        @pl.when(local == 2 + at)
        def _():
            write(theirs, low_theirs, at)


SMEM = pl.BlockSpec(memory_space=pltpu.SMEM)
VMEM = pl.BlockSpec(memory_space=pltpu.VMEM)
ANY = pl.BlockSpec(memory_space=pl.ANY)
MIB = 1 << 20


def near(*arrays):
    return [pltpu.with_memory_space_constraint(a, pltpu.VMEM) for a in arrays]


def call(kernel, in_specs, out_shape, out_specs=None, grid=(), scratch=(), flops=0, limit=16, aliases=None):
    if out_specs is None:
        out_specs = jax.tree.map(lambda _: VMEM, out_shape, is_leaf=lambda x: not isinstance(x, (list, tuple)))
    return pl.pallas_call(
        kernel,
        grid=grid,
        in_specs=in_specs,
        out_specs=out_specs,
        out_shape=out_shape,
        scratch_shapes=scratch,
        input_output_aliases=aliases or {},
        cost_estimate=pl.CostEstimate(flops=flops, transcendentals=0, bytes_accessed=MIB),
        compiler_params=pltpu.CompilerParams(
            dimension_semantics=("arbitrary",) * len(grid), vmem_limit_bytes=limit * MIB
        ),
    )


def far(dims, dtype=BF):
    return jax.ShapeDtypeStruct(dims, dtype)


def shape(dims, dtype=BF):
    return pltpu.VMEM(dims, dtype)


def held(*arrays):
    return [pltpu.with_memory_space_constraint(a, pltpu.HBM) for a in arrays]


def body(hidden_in, w_query, w_key, w_value, lengths, owners):
    swap = [(0, 1), (1, 0)]
    half = (2, OWN * ROWS, HD)
    packed = OWN * ROWS

    q, k, v, send, keep, picks = call(
        project_kernel,
        [ANY] * 6,
        [
            shape((4, SPAN, 128)),
            shape((4, SPAN, 128)),
            shape((4, SPAN, 512)),
            shape(half),
            shape(half),
            shape((2, packed, 128)),
        ],
        scratch=[
            pltpu.VMEM((4, SPAN, D), BF),
            pltpu.VMEM((D, 512), BF),
            pltpu.VMEM((D, 256), BF),
            pltpu.SMEM((4,), jnp.int32),
            pltpu.SemaphoreType.DMA((D // CHUNK, 4)),
            pltpu.SemaphoreType.DMA((3,)),
            pltpu.SemaphoreType.DMA((2,)),
        ],
        flops=3_000_000_000,
        limit=24,
    )(*held(lengths, hidden_in, w_value, w_query, w_key, jnp.asarray(PICKS, BF)))

    recv = lax.ppermute(send, "c", swap)
    lines = jnp.asarray(LINES)
    own_shapes = [shape((4, SPAN, 512), F32), shape((4, SPAN, 128), F32), shape((4, OWN, SPAN, ROWS))]
    num, den, feats = call(self_kernel, [SMEM] + [VMEM] * 5, own_shapes, flops=3_000_000_000)(
        lengths, *near(q, k, v, picks, lines)
    )
    pair = call(pair_kernel, [VMEM, VMEM, ANY], shape((CHIPS, SLICE, HD)))(*near(keep, recv, den))
    pieces = lax.all_to_all(pair, CHIP, 0, 0)
    both = call(scan_kernel, [SMEM, VMEM], shape((CHIPS, 2 * SLICE, HD)))(owners, *near(pieces))
    back = lax.all_to_all(both, CHIP, 0, 0)
    own_state, given = call(
        prefix_kernel, [VMEM] * 3, [shape(half), shape((STATE + 2 * OWN * LOW_ROWS, HD))]
    )(*near(back, keep, recv))
    taken = lax.ppermute(given, "c", swap)
    num, den, feats = call(
        late_kernel,
        [SMEM] + [VMEM] * 8 + [ANY],
        own_shapes,
        flops=3_000_000_000,
        aliases={6: 0, 7: 1, 8: 2},
    )(lengths, *near(q, k, v, picks, lines, num, den, feats, own_state))

    own_att, square = call(
        own_kernel,
        [SMEM] + [VMEM] * 4,
        [shape((2, SPAN, 512), F32), shape((8, HD), F32)],
        flops=500_000_000,
    )(lengths, *near(own_state, num, den, feats))
    other_att, sent = call(
        other_kernel,
        [SMEM] + [VMEM] * 7,
        [shape((2, SPAN, 512), F32), shape((4, SENT, HD))],
        flops=500_000_000,
    )(lengths, *near(taken, num, den, feats, square, back, jnp.asarray(SPREAD, BF)))
    mine = lax.all_to_all(sent, "feat", 0, 0)
    theirs = lax.ppermute(mine, "c", swap)
    mixed = call(
        mix_kernel,
        [VMEM] * 3,
        far((4, SPAN, 512)),
        pl.BlockSpec((1, SPAN, 512), lambda i: ((i + 2 * lax.axis_index("c")) % 4, 0, 0)),
        (4,),
        flops=500_000_000,
    )(*near(own_att, other_att, mine))

    quad, low_out, norm_quad, norm_low = call(
        final_kernel,
        [SMEM] + [VMEM] * 4,
        [
            far((1, 4, H, 64, HD), F32),
            far((1, 4, FD + 1, OWN, HD), F32),
            far((1, 4, H, 64), F32),
            far((1, 4, OWN, FD + 1), F32),
        ],
        [
            pl.BlockSpec((1, 1, H, 64, HD), lambda i: (0, i, 0, 0, 0)),
            pl.BlockSpec((1, 1, FD + 1, OWN, HD), lambda i: (0, i, 0, 0, 0)),
            pl.BlockSpec((1, 1, H, 64), lambda i: (0, i, 0, 0)),
            pl.BlockSpec((1, 1, OWN, FD + 1), lambda i: (0, i, 0, 0)),
        ],
        (4,),
    )(owners, *near(mine, theirs, given, taken))
    return mixed, quad, jnp.transpose(low_out, (0, 1, 3, 2, 4)), norm_quad, norm_low


def solution(mesh):
    torus = Mesh(mesh.devices.reshape(8, 4, 2, 4), ("z", "y", "c", "feat"))
    seq = ("z", "y", "c")
    return jax.shard_map(
        body,
        mesh=torus,
        in_specs=(P(None, seq, None), P(), P(), P(None, "feat"), P(), P()),
        out_specs=(
            P(None, seq, "feat"),
            P(seq, None, None, "feat", None),
            P(seq, None, "feat", None, None),
            P(seq, None, None, "feat"),
            P(seq, None, "feat", None),
        ),
        check_vma=False,
    )
```

```python
import functools

import jax
import jax.numpy as jnp
import numpy as np
from jax import lax
from jax.experimental import pallas as pl
from jax.experimental.pallas import tpu as pltpu
from jax.sharding import Mesh
from jax.sharding import PartitionSpec as P

H = 16
FD = 16
HD = 128
D = 2048
SPAN = 256
OWN = 4
ROWS = 160
QUADS = 136
LOW = 128
NORM = 153
CHIPS = 32
SLICE = 2 * OWN * ROWS // CHIPS
NORM_FLOOR = 0.0001
BF = jnp.bfloat16
F32 = jnp.float32
CHIP = ("z", "y")


def feature_rows():
    pairs = [(i, j) for i in range(FD) for j in range(i, FD)]
    rows = [u if u < LOW else u + FD + 1 for u in range(QUADS)]
    return pairs, rows


def tables():
    pairs, rows = feature_rows()
    first = np.zeros((ROWS, FD), np.float32)
    second = np.zeros((ROWS, FD), np.float32)
    spread = np.zeros((FD * FD, ROWS), np.float32)
    for (i, j), row in zip(pairs, rows):
        first[row, i] = 1
        second[row, j] = 1
        spread[i * FD + j, row] = 1
        spread[j * FD + i, row] = 1
    for i in range(FD):
        first[LOW + 1 + i, i] = 1
    picks = np.zeros((2, 2, OWN, ROWS, 2 * OWN * FD), np.float32)
    for half in range(2):
        for head in range(OWN):
            at = half * OWN * FD + head * FD
            picks[half, 0, head, :, at : at + FD] = first
            picks[half, 1, head, :, at : at + FD] = second
    lines = np.zeros((8, ROWS), np.float32)
    for (i, j), row in zip(pairs, rows):
        lines[0, row] = (1.0 if i == j else 2.0) * (2.0 * FD) ** -0.5
    lines[0, LOW + 1 : LOW + 1 + FD] = lines[1, LOW + 1 : LOW + 1 + FD] = FD**-0.25
    lines[:3, LOW] = 1.0
    return picks.reshape(2, 2, OWN * ROWS, 2 * OWN * FD), spread, lines


PICKS, SPREAD, LINES = tables()


def is_low(row):
    return (row >= LOW) & (row <= LOW + FD)


def nt(a, b):
    return lax.dot_general(a, b, (((1,), (1,)), ((), ())), preferred_element_type=F32)


def place():
    core = lax.axis_index("c")
    chip = lax.axis_index("z") * 4 + lax.axis_index("y")
    return core, chip, chip * 2 + core, lax.axis_index("feat")


CHUNK = 512
AHEAD = 5


def project_kernel(
    lens_h, hid, wv, wq, wk, picks_h, q_o, k_o, v_o, send_o, keep_o, picks, hid_b, wv_b, wqk_b, lens, sems, rest, small
):
    core, _, seq, feat = place()
    lanes = pl.ds(pl.multiple_of(feat // 2 * 128, 128), 128)
    first = (2 + 2 * core) % 4
    queue = []
    for n in range(D // CHUNK):
        rows = pl.ds(n * CHUNK, CHUNK)
        queue.append(
            [
                pltpu.make_async_copy(hid.at[first, :, rows], hid_b.at[2, :, rows], sems.at[n, 0]),
                pltpu.make_async_copy(wq.at[rows, lanes], wqk_b.at[rows, :128], sems.at[n, 1]),
                pltpu.make_async_copy(wk.at[rows, lanes], wqk_b.at[rows, 128:], sems.at[n, 2]),
                pltpu.make_async_copy(wv.at[rows], wv_b.at[rows], sems.at[n, 3]),
            ]
        )
    queue.append(
        [
            pltpu.make_async_copy(lens_h, lens, small.at[0]),
            pltpu.make_async_copy(picks_h.at[feat % 2], picks, small.at[1]),
        ]
    )
    for n, local in enumerate((3, 0, 1)):
        queue.append([pltpu.make_async_copy(hid.at[(local + 2 * core) % 4], hid_b.at[local], rest.at[n])])

    def start(n):
        if n < len(queue):
            for copy in queue[n]:
                copy.start()

    def arrive(n):
        for copy in queue[n]:
            copy.wait()
        start(n + AHEAD)

    for n in range(AHEAD):
        start(n)
    row = lax.broadcasted_iota(jnp.int32, (ROWS, SPAN), 0)
    low = is_low(row)
    const = (row == LOW).astype(F32)
    fixed = jnp.where(row == LOW, 1.0, jnp.where(low, FD**-0.25, (2.0 * FD) ** -0.5))
    ones = jnp.ones((8, SPAN), BF)
    tail_row = lax.broadcasted_iota(jnp.int32, (8, HD), 0) + (ROWS - 8)

    def project(n, local):
        if n == 0:
            v = jnp.zeros((SPAN, 512), F32)
            qk = jnp.zeros((SPAN, 256), F32)
            for m in range(D // CHUNK):
                arrive(m)
                rows = slice(m * CHUNK, (m + 1) * CHUNK)
                x = hid_b[local, :, rows]
                qk = qk + jnp.dot(x, wqk_b[rows], preferred_element_type=F32)
                v = v + jnp.dot(x, wv_b[rows], preferred_element_type=F32)
            arrive(D // CHUNK)
        else:
            arrive(D // CHUNK + n)
            x = hid_b[local]
            qk = jnp.dot(x, wqk_b[...], preferred_element_type=F32)
            v = jnp.dot(x, wv_b[...], preferred_element_type=F32)
        q_o[local] = qk[:, :128].astype(BF)
        k_o[local] = qk[:, 128:].astype(BF)
        v_o[local] = v.astype(BF)

    def states(local):
        key_t = k_o[local].astype(F32).T.astype(BF)
        token = seq * SPAN + lax.broadcasted_iota(jnp.int32, (1, SPAN), 1)
        scale = jnp.where(token < lens[(local + 2 * core) % 4], fixed, 0.0)
        bias = jnp.where(low, scale, 0.0)
        target = send_o if local >= 2 else keep_o
        for h in range(OWN):
            at = h * ROWS
            u = jnp.dot(picks[0, at : at + ROWS], key_t, preferred_element_type=F32)
            w = jnp.dot(picks[1, at : at + ROWS], key_t, preferred_element_type=F32)
            feats = ((u + const) * (w * scale + bias)).astype(BF)
            state = jnp.dot(feats, v_o[local, :, h * HD : (h + 1) * HD], preferred_element_type=F32)
            norm = nt(ones, feats)
            rest_norm = jnp.concatenate([norm[:, HD:], jnp.zeros((8, 2 * HD - ROWS), F32)], axis=1)
            tail = state[ROWS - 8 :]
            tail = jnp.where(tail_row == NORM, norm[:, :HD], jnp.where(tail_row == NORM + 1, rest_norm, tail))
            target[local % 2, at : at + ROWS] = jnp.concatenate([state[: ROWS - 8], tail], axis=0).astype(BF)

    order = (2, 3, 0, 1)
    for n in range(5):
        if n < 4:
            project(n, order[n])
        if n > 0:
            states(order[n - 1])


def self_kernel(lens, q, k, v, picks, lines, num_o, den_o, feat_o, late=False):
    core, _, seq, feat = place()
    z = lax.axis_index("z")
    early = jnp.where(z < 4, 5 - z, 0) + (lax.axis_index("y") == 0).astype(jnp.int32)
    split = jnp.minimum(early, 4)
    tq = lax.broadcasted_iota(jnp.int32, (SPAN, SPAN), 0)
    tk = lax.broadcasted_iota(jnp.int32, (SPAN, SPAN), 1)
    lane = lax.broadcasted_iota(jnp.int32, (SPAN, HD), 1)
    scale, bias, const = lines[0:1], lines[1:2], lines[2:3]
    ones = jnp.ones((SPAN, HD), BF)

    def prompt(local, _):
        query = q[local]
        key = k[local]
        seen = (tk <= tq) & (seq * SPAN + tk < lens[(local + 2 * core) % 4])
        den_all = jnp.zeros((SPAN, HD), F32)
        for h in range(OWN):
            at = h * ROWS
            mine = jnp.where(lane // FD == feat % 2 * OWN + h, query, jnp.zeros_like(query))
            score = nt(mine, key)
            weight = jnp.where(seen, 1.0 + score * (FD**-0.5) + score * score * (0.5 / FD), 0.0).astype(BF)
            value = jnp.concatenate([v[local, :, h * HD : (h + 1) * HD], ones], axis=1)
            both = jnp.dot(weight, value, preferred_element_type=F32)
            num_o[local, :, h * HD : (h + 1) * HD] = both[:, :HD]
            den_all = jnp.where(lane == h, both[:, HD:], den_all)
            u = nt(query, picks[0, at : at + ROWS])
            w = nt(query, picks[1, at : at + ROWS])
            feat_o[local, h] = ((u + const) * (w * scale + bias)).astype(BF)
        den_o[local] = den_all
        return _

    lax.fori_loop(split if late else 0, 4 if late else split, prompt, 0)


def pair_kernel(keep, recv, after, out):
    pair = (keep[...].astype(F32) + recv[...].astype(F32)).astype(BF)
    out[...] = pair.reshape(CHIPS, SLICE, HD)


def scan_kernel(owners, pieces, out):
    core, chip, _, _ = place()
    home = owners[2 * core + chip // 16] // 2
    before = jnp.zeros((SLICE, HD), F32)
    for n in range(CHIPS):
        out[n, :SLICE] = before.astype(BF)
        before = before + pieces[n].astype(F32)
    total = before.astype(BF)
    nothing = jnp.zeros_like(total)
    for n in range(CHIPS):
        out[n, SLICE:] = jnp.where(home == n, total, nothing)


STATE = 2 * OWN * ROWS
LOW_ROWS = ROWS - LOW
WIDE = 2 * OWN * 64
NORMS = WIDE + 8
SENT = NORMS + 16


def prefix_kernel(back, keep, recv, own_o, other_o):
    before = back[:, :SLICE].reshape(STATE, HD).astype(F32)
    second = lax.axis_index("c") == 1
    added = jnp.where(second, recv[...], keep[...]).reshape(STATE, HD).astype(F32)
    both = (before + added).astype(BF)
    plain = before.astype(BF)
    own_o[...] = jnp.where(second, both, plain)
    other_o[:STATE] = jnp.where(second, plain, both)
    total = back[:, SLICE:].reshape(2 * OWN, ROWS, HD)
    other_o[STATE:] = total[:, LOW:].reshape(2 * OWN * LOW_ROWS, HD)


def norm_row(part):
    return jnp.concatenate([part[NORM : NORM + 1], part[NORM + 1 : NORM + 2, : ROWS - HD]], axis=1)


def spread_kernel(back, table, out):
    total = back[:, SLICE:].reshape(2 * OWN, ROWS, HD)
    for n in range(2 * OWN):
        wide = jnp.dot(table[...], total[n], preferred_element_type=F32).astype(BF)
        for f in range(4):
            out[f, n * 64 : (n + 1) * 64] = wide[f * 64 : (f + 1) * 64]
    norm = nt(jnp.concatenate([norm_row(total[n]) for n in range(2 * OWN)], axis=0), table[...])
    pad = jnp.zeros((8, 64), F32)
    for f in range(4):
        out[f, WIDE:NORMS] = jnp.concatenate([norm[:, f * 64 : (f + 1) * 64], pad], axis=1).astype(BF)


def attend(first, lens, state, num, den, feat, att_o):
    core, _, seq, _ = place()
    token = seq * SPAN + lax.broadcasted_iota(jnp.int32, (SPAN, HD), 0)
    ones = jnp.ones((8, HD), F32)
    found = []
    for n in range(2):
        live = token < lens[(first + n + 2 * core) % 4]
        den_all = den[first + n]
        squares = jnp.zeros((SPAN, HD), F32)
        for h in range(OWN):
            feats = feat[first + n, h]
            part = state(n, h)
            total = num[first + n, :, h * HD : (h + 1) * HD] + jnp.dot(feats, part, preferred_element_type=F32)
            below = nt(feats, jnp.broadcast_to(norm_row(part), (HD, ROWS))) + den_all[:, h : h + 1]
            att = jnp.where(live, total / below, 0.0)
            att_o[n, :, h * HD : (h + 1) * HD] = att
            squares = squares + att * att
        sums = lax.dot_general(
            ones,
            squares,
            (((1,), (1,)), ((), ())),
            precision=lax.Precision.HIGHEST,
            preferred_element_type=F32,
        )
        found += [sums[:1, :HD], sums[:1, HD:]]
    return found


def part_of(state):
    def part(n, h):
        at = (n * OWN + h) * ROWS
        return state[at : at + ROWS]

    return part


def own_kernel(
    lens, state, q, k, v, picks, lines, num_i, den_i, feat_i, num, den, feat, att_o, square_o, quad_o, blank, sem
):
    blank[...] = jnp.zeros_like(blank)
    clear = [pltpu.make_async_copy(blank, quad_o.at[0, n], sem.at[n]) for n in range(4)]
    for copy in clear:
        copy.start()
    self_kernel(lens, q, k, v, picks, lines, num, den, feat, late=True)
    found = attend(0, lens, part_of(state), num, den, feat, att_o)
    square_o[...] = jnp.concatenate(found + [jnp.zeros((4, HD), F32)], axis=0)
    for copy in clear:
        copy.wait()


def other_kernel(lens, state, num, den, feat, square, sent_i, att_o, sent_o):
    found = attend(2, lens, part_of(state), num, den, feat, att_o)
    squares = jnp.concatenate([square[:4]] + found, axis=0)
    high = squares.astype(BF)
    rest = (squares - high.astype(F32)).astype(BF)
    for f in range(4):
        sent_o[f, NORMS : NORMS + 8] = high
        sent_o[f, NORMS + 8 :] = rest


def mix_kernel(own, other, sent, mixed_o, block, sem):
    core = lax.axis_index("c")
    square = jnp.zeros((8, HD), F32)
    for f in range(4):
        square = square + (sent[f, NORMS : NORMS + 8].astype(F32) + sent[f, NORMS + 8 :].astype(F32))
    factor = lax.rsqrt(square * (1.0 / D) + NORM_FLOOR).T
    copies = []
    for local in range(4):
        source = own if local < 2 else other
        for k in range(2):
            column = factor[:, 2 * local + k : 2 * local + k + 1]
            rows = slice(k * HD, (k + 1) * HD)
            block[local, rows] = (source[local % 2, rows] * column).astype(BF)
        copies.append(pltpu.make_async_copy(block.at[local], mixed_o.at[(local + 2 * core) % 4], sem.at[local]))
        copies[-1].start()
    for copy in copies:
        copy.wait()


def final_kernel(
    owners, mine, theirs, low_mine, low_theirs, cleared, quad_o, low_o, nquad_o, nlow_o, block, low_b, nquad_b, nlow_b, sem
):
    core, _, seq, _ = place()
    low_b[...] = jnp.zeros_like(low_b)
    nquad_b[...] = jnp.zeros_like(nquad_b)
    nlow_b[...] = jnp.zeros_like(nlow_b)

    def move(local, f):
        heads = pl.ds(f * OWN, OWN)
        prompt = (local + 2 * core) % 4
        return pltpu.make_async_copy(block.at[local, heads], quad_o.at[0, prompt, heads], sem.at[local, f])

    for local in range(4):
        prompt = (local + 2 * core) % 4
        wide, low = (mine, low_mine) if local < 2 else (theirs, low_theirs)
        at = local % 2

        @pl.when(owners[prompt] == seq)
        def _():
            for f in range(4):
                for h in range(OWN):
                    row = (at * OWN + h) * 64
                    block[local, f * OWN + h] = wide[f, row : row + 64].astype(F32)
                move(local, f).start()
            for f in range(4):
                for h in range(OWN):
                    row = WIDE + at * OWN + h
                    nquad_b[prompt, f * OWN + h : f * OWN + h + 1] = wide[f, row : row + 1].astype(F32)[:, :64]
            for h in range(OWN):
                row = STATE + (at * OWN + h) * LOW_ROWS
                piece = low[row : row + LOW_ROWS].astype(F32)
                for r in range(FD + 1):
                    low_b[prompt, r, h : h + 1] = piece[r : r + 1]
                at_norm = NORM + 1 - LOW
                nlow_b[prompt, h : h + 1] = piece[at_norm : at_norm + 1, : FD + 1]

    small = [
        pltpu.make_async_copy(low_b, low_o.at[0], sem.at[4, 0]),
        pltpu.make_async_copy(nquad_b, nquad_o.at[0], sem.at[4, 1]),
        pltpu.make_async_copy(nlow_b, nlow_o.at[0], sem.at[4, 2]),
    ]
    for copy in small:
        copy.start()
    for local in range(4):

        @pl.when(owners[(local + 2 * core) % 4] == seq)
        def _():
            for f in range(4):
                move(local, f).wait()

    for copy in small:
        copy.wait()


SMEM = pl.BlockSpec(memory_space=pltpu.SMEM)
VMEM = pl.BlockSpec(memory_space=pltpu.VMEM)
ANY = pl.BlockSpec(memory_space=pl.ANY)
MIB = 1 << 20


def near(*arrays):
    return [pltpu.with_memory_space_constraint(a, pltpu.VMEM) for a in arrays]


def call(kernel, in_specs, out_shape, out_specs=None, grid=(), scratch=(), flops=0, limit=16, aliases=None):
    if out_specs is None:
        out_specs = jax.tree.map(lambda _: VMEM, out_shape, is_leaf=lambda x: not isinstance(x, (list, tuple)))
    return pl.pallas_call(
        kernel,
        grid=grid,
        in_specs=in_specs,
        out_specs=out_specs,
        out_shape=out_shape,
        scratch_shapes=scratch,
        input_output_aliases=aliases or {},
        cost_estimate=pl.CostEstimate(flops=flops, transcendentals=0, bytes_accessed=MIB),
        compiler_params=pltpu.CompilerParams(
            dimension_semantics=("arbitrary",) * len(grid), vmem_limit_bytes=limit * MIB
        ),
    )


def far(dims, dtype=BF):
    return jax.ShapeDtypeStruct(dims, dtype)


def shape(dims, dtype=BF):
    return pltpu.VMEM(dims, dtype)


def held(*arrays):
    return [pltpu.with_memory_space_constraint(a, pltpu.HBM) for a in arrays]


def body(hidden_in, w_query, w_key, w_value, lengths, owners):
    swap = [(0, 1), (1, 0)]
    half = (2, OWN * ROWS, HD)
    packed = OWN * ROWS

    q, k, v, send, keep, picks = call(
        project_kernel,
        [ANY] * 6,
        [
            shape((4, SPAN, 128)),
            shape((4, SPAN, 128)),
            shape((4, SPAN, 512)),
            shape(half),
            shape(half),
            shape((2, packed, 128)),
        ],
        scratch=[
            pltpu.VMEM((4, SPAN, D), BF),
            pltpu.VMEM((D, 512), BF),
            pltpu.VMEM((D, 256), BF),
            pltpu.SMEM((4,), jnp.int32),
            pltpu.SemaphoreType.DMA((D // CHUNK, 4)),
            pltpu.SemaphoreType.DMA((3,)),
            pltpu.SemaphoreType.DMA((2,)),
        ],
        flops=3_000_000_000,
        limit=24,
    )(*held(lengths, hidden_in, w_value, w_query, w_key, jnp.asarray(PICKS, BF)))

    recv = lax.ppermute(send, "c", swap)
    lines = jnp.asarray(LINES)
    own_shapes = [shape((4, SPAN, 512), F32), shape((4, SPAN, 128), F32), shape((4, OWN, SPAN, ROWS))]
    num, den, feats = call(self_kernel, [SMEM] + [VMEM] * 5, own_shapes, flops=3_000_000_000)(
        lengths, *near(q, k, v, picks, lines)
    )
    pair = call(pair_kernel, [VMEM, VMEM, ANY], shape((CHIPS, SLICE, HD)))(*near(keep, recv, den))
    pieces = lax.all_to_all(pair, CHIP, 0, 0)
    both = call(scan_kernel, [SMEM, VMEM], shape((CHIPS, 2 * SLICE, HD)))(owners, *near(pieces))
    back = lax.all_to_all(both, CHIP, 0, 0)
    own_state, given = call(
        prefix_kernel, [VMEM] * 3, [shape((STATE, HD)), shape((STATE + 2 * OWN * LOW_ROWS, HD))]
    )(*near(back, keep, recv))
    taken = lax.ppermute(given, "c", swap)
    num, den, feats, own_att, square, quad = call(
        own_kernel,
        [SMEM] + [VMEM] * 9,
        own_shapes + [shape((2, SPAN, 512), F32), shape((8, HD), F32), pltpu.HBM((1, 4, H, 64, HD), F32)],
        [VMEM] * 5 + [ANY],
        scratch=[pltpu.VMEM((H, 64, HD), F32), pltpu.SemaphoreType.DMA((4,))],
        flops=3_000_000_000,
        aliases={7: 0, 8: 1, 9: 2},
    )(lengths, *near(own_state, q, k, v, picks, lines, num, den, feats))
    sent = call(spread_kernel, [VMEM] * 2, shape((4, SENT, HD)), flops=500_000_000)(
        *near(back, jnp.asarray(SPREAD, BF))
    )
    other_att, sent = call(
        other_kernel,
        [SMEM] + [VMEM] * 6,
        [shape((2, SPAN, 512), F32), shape((4, SENT, HD))],
        flops=500_000_000,
        aliases={6: 1},
    )(lengths, *near(taken, num, den, feats, square, sent))
    mine = lax.all_to_all(sent, "feat", 0, 0)
    theirs = lax.ppermute(mine, "c", swap)
    mixed = call(
        mix_kernel,
        [VMEM] * 3,
        pltpu.HBM((4, SPAN, 512), BF),
        ANY,
        scratch=[pltpu.VMEM((4, SPAN, 512), BF), pltpu.SemaphoreType.DMA((4,))],
        flops=500_000_000,
    )(*near(own_att, other_att, mine))

    quad, low_out, norm_quad, norm_low = call(
        final_kernel,
        [SMEM] + [VMEM] * 4 + [ANY],
        [
            pltpu.HBM((1, 4, H, 64, HD), F32),
            pltpu.HBM((1, 4, FD + 1, OWN, HD), F32),
            pltpu.HBM((1, 4, H, 64), F32),
            pltpu.HBM((1, 4, OWN, FD + 1), F32),
        ],
        [ANY] * 4,
        scratch=[
            pltpu.VMEM((4, H, 64, HD), F32),
            pltpu.VMEM((4, FD + 1, OWN, HD), F32),
            pltpu.VMEM((4, H, 64), F32),
            pltpu.VMEM((4, OWN, FD + 1), F32),
            pltpu.SemaphoreType.DMA((5, 4)),
        ],
        aliases={5: 0},
    )(owners, *near(mine, theirs, given, taken), *held(quad))
    return mixed, quad, jnp.transpose(low_out, (0, 1, 3, 2, 4)), norm_quad, norm_low


def solution(mesh):
    torus = Mesh(mesh.devices.reshape(8, 4, 2, 4), ("z", "y", "c", "feat"))
    seq = ("z", "y", "c")
    return jax.shard_map(
        body,
        mesh=torus,
        in_specs=(P(None, seq, None), P(), P(), P(None, "feat"), P(), P()),
        out_specs=(
            P(None, seq, "feat"),
            P(seq, None, None, "feat", None),
            P(seq, None, "feat", None, None),
            P(seq, None, None, "feat"),
            P(seq, None, "feat", None),
        ),
        check_vma=False,
    )
```

```python
import functools

import jax
import jax.numpy as jnp
import numpy as np
from jax import lax
from jax.experimental import pallas as pl
from jax.experimental.pallas import tpu as pltpu
from jax.sharding import Mesh
from jax.sharding import PartitionSpec as P

H = 16
FD = 16
HD = 128
D = 2048
SPAN = 256
OWN = 4
ROWS = 160
QUADS = 136
LOW = 128
NORM = 153
CHIPS = 32
SLICE = 2 * OWN * ROWS // CHIPS
NORM_FLOOR = 0.0001
BF = jnp.bfloat16
F32 = jnp.float32
CHIP = ("z", "y")


def feature_rows():
    pairs = [(i, j) for i in range(FD) for j in range(i, FD)]
    rows = [u if u < LOW else u + FD + 1 for u in range(QUADS)]
    return pairs, rows


def tables():
    pairs, rows = feature_rows()
    first = np.zeros((ROWS, FD), np.float32)
    second = np.zeros((ROWS, FD), np.float32)
    spread = np.zeros((FD * FD, ROWS), np.float32)
    for (i, j), row in zip(pairs, rows):
        first[row, i] = 1
        second[row, j] = 1
        spread[i * FD + j, row] = 1
        spread[j * FD + i, row] = 1
    for i in range(FD):
        first[LOW + 1 + i, i] = 1
    picks = np.zeros((2, 2, OWN, ROWS, 2 * OWN * FD), np.float32)
    for half in range(2):
        for head in range(OWN):
            at = half * OWN * FD + head * FD
            picks[half, 0, head, :, at : at + FD] = first
            picks[half, 1, head, :, at : at + FD] = second
    lines = np.zeros((8, ROWS), np.float32)
    for (i, j), row in zip(pairs, rows):
        lines[0, row] = (1.0 if i == j else 2.0) * (2.0 * FD) ** -0.5
    lines[0, LOW + 1 : LOW + 1 + FD] = lines[1, LOW + 1 : LOW + 1 + FD] = FD**-0.25
    lines[:3, LOW] = 1.0
    return picks.reshape(2, 2, OWN * ROWS, 2 * OWN * FD), spread, lines


PICKS, SPREAD, LINES = tables()


def is_low(row):
    return (row >= LOW) & (row <= LOW + FD)


def nt(a, b):
    return lax.dot_general(a, b, (((1,), (1,)), ((), ())), preferred_element_type=F32)


def place():
    core = lax.axis_index("c")
    chip = lax.axis_index("z") * 4 + lax.axis_index("y")
    return core, chip, chip * 2 + core, lax.axis_index("feat")


CHUNK = 512
AHEAD = 5


def project_kernel(lens_h, hid, wv, wq, wk, picks_h, q_o, k_o, v_o, send_o, picks, hid_b, wv_b, wqk_b, lens, sems, rest, small):
    core, _, seq, feat = place()
    lanes = pl.ds(pl.multiple_of(feat // 2 * 128, 128), 128)
    first = (2 + 2 * core) % 4
    queue = []
    for n in range(D // CHUNK):
        rows = pl.ds(n * CHUNK, CHUNK)
        queue.append(
            [
                pltpu.make_async_copy(hid.at[first, :, rows], hid_b.at[2, :, rows], sems.at[n, 0]),
                pltpu.make_async_copy(wq.at[rows, lanes], wqk_b.at[rows, :128], sems.at[n, 1]),
                pltpu.make_async_copy(wk.at[rows, lanes], wqk_b.at[rows, 128:], sems.at[n, 2]),
                pltpu.make_async_copy(wv.at[rows], wv_b.at[rows], sems.at[n, 3]),
            ]
        )
    queue.append(
        [
            pltpu.make_async_copy(lens_h, lens, small.at[0]),
            pltpu.make_async_copy(picks_h.at[feat % 2], picks, small.at[1]),
        ]
    )
    for n, local in enumerate((3, 0, 1)):
        queue.append([pltpu.make_async_copy(hid.at[(local + 2 * core) % 4], hid_b.at[local], rest.at[n])])

    def start(n):
        if n < len(queue):
            for copy in queue[n]:
                copy.start()

    def arrive(n):
        for copy in queue[n]:
            copy.wait()
        start(n + AHEAD)

    for n in range(AHEAD):
        start(n)
    def first_product():
        v = jnp.zeros((SPAN, 512), F32)
        qk = jnp.zeros((SPAN, 256), F32)
        for m in range(D // CHUNK):
            arrive(m)
            rows = slice(m * CHUNK, (m + 1) * CHUNK)
            x = hid_b[2, :, rows]
            qk = qk + jnp.dot(x, wqk_b[rows], preferred_element_type=F32)
            v = v + jnp.dot(x, wv_b[rows], preferred_element_type=F32)
        arrive(D // CHUNK)
        return qk, v

    keep_rows(0, first_product(), q_o, k_o, v_o)
    arrive(D // CHUNK + 1)
    keep_rows(1, product(hid_b[3], wqk_b, wv_b), q_o, k_o, v_o)
    states(0, 2, lens, k_o, v_o, picks, send_o)
    states(1, 3, lens, k_o, v_o, picks, send_o)
    for n in range(2, 4):
        arrive(D // CHUNK + n)


def product(x, wqk, wv):
    return (
        jnp.dot(x, wqk[...], preferred_element_type=F32),
        jnp.dot(x, wv[...], preferred_element_type=F32),
    )


def keep_rows(n, products, q_o, k_o, v_o):
    qk, v = products
    q_o[n] = qk[:, :128].astype(BF)
    k_o[n] = qk[:, 128:].astype(BF)
    v_o[n] = v.astype(BF)


def states(n, local, lens, k, v, picks, out):
    core, _, seq, _ = place()
    row = lax.broadcasted_iota(jnp.int32, (ROWS, SPAN), 0)
    low = is_low(row)
    const = (row == LOW).astype(F32)
    fixed = jnp.where(row == LOW, 1.0, jnp.where(low, FD**-0.25, (2.0 * FD) ** -0.5))
    ones = jnp.ones((8, SPAN), BF)
    tail_row = lax.broadcasted_iota(jnp.int32, (8, HD), 0) + (ROWS - 8)
    key_t = k[n].astype(F32).T.astype(BF)
    token = seq * SPAN + lax.broadcasted_iota(jnp.int32, (1, SPAN), 1)
    scale = jnp.where(token < lens[(local + 2 * core) % 4], fixed, 0.0)
    bias = jnp.where(low, scale, 0.0)
    for h in range(OWN):
        at = h * ROWS
        u = jnp.dot(picks[0, at : at + ROWS], key_t, preferred_element_type=F32)
        w = jnp.dot(picks[1, at : at + ROWS], key_t, preferred_element_type=F32)
        feats = ((u + const) * (w * scale + bias)).astype(BF)
        state = jnp.dot(feats, v[n, :, h * HD : (h + 1) * HD], preferred_element_type=F32)
        norm = nt(ones, feats)
        rest_norm = jnp.concatenate([norm[:, HD:], jnp.zeros((8, 2 * HD - ROWS), F32)], axis=1)
        tail = state[ROWS - 8 :]
        tail = jnp.where(tail_row == NORM, norm[:, :HD], jnp.where(tail_row == NORM + 1, rest_norm, tail))
        out[n, at : at + ROWS] = jnp.concatenate([state[: ROWS - 8], tail], axis=0).astype(BF)


def keep_kernel(lens, hid, wqk, wv, picks, qb, kb, vb, lines, qa, ka, va, keep_o, num_o, den_o, feat_o):
    keep_rows(0, product(hid[0], wqk, wv), qa, ka, va)
    keep_rows(1, product(hid[1], wqk, wv), qa, ka, va)
    states(0, 0, lens, ka, va, picks, keep_o)
    states(1, 1, lens, ka, va, picks, keep_o)
    self_kernel(lens, (qa, ka, va), (qb, kb, vb), picks, lines, num_o, den_o, feat_o)


def self_kernel(lens, own, other, picks, lines, num_o, den_o, feat_o, late=False):
    core, _, seq, feat = place()
    z = lax.axis_index("z")
    early = jnp.where(z < 4, 5 - z, 0) + (lax.axis_index("y") == 0).astype(jnp.int32)
    split = jnp.minimum(early, 4)
    tq = lax.broadcasted_iota(jnp.int32, (SPAN, SPAN), 0)
    tk = lax.broadcasted_iota(jnp.int32, (SPAN, SPAN), 1)
    lane = lax.broadcasted_iota(jnp.int32, (SPAN, HD), 1)
    scale, bias, const = lines[0:1], lines[1:2], lines[2:3]
    ones = jnp.ones((SPAN, HD), BF)

    def prompt(local, _, q, k, v):
        query = q[local % 2]
        key = k[local % 2]
        seen = (tk <= tq) & (seq * SPAN + tk < lens[(local + 2 * core) % 4])
        den_all = jnp.zeros((SPAN, HD), F32)
        for h in range(OWN):
            at = h * ROWS
            mine = jnp.where(lane // FD == feat % 2 * OWN + h, query, jnp.zeros_like(query))
            score = nt(mine, key)
            weight = jnp.where(seen, 1.0 + score * (FD**-0.5) + score * score * (0.5 / FD), 0.0).astype(BF)
            value = jnp.concatenate([v[local % 2, :, h * HD : (h + 1) * HD], ones], axis=1)
            both = jnp.dot(weight, value, preferred_element_type=F32)
            num_o[local, :, h * HD : (h + 1) * HD] = both[:, :HD]
            den_all = jnp.where(lane == h, both[:, HD:], den_all)
            u = nt(query, picks[0, at : at + ROWS])
            w = nt(query, picks[1, at : at + ROWS])
            feat_o[local, h] = ((u + const) * (w * scale + bias)).astype(BF)
        den_o[local] = den_all
        return _

    for half, refs in ((0, own), (1, other)):
        cut = jnp.clip(split - 2 * half, 0, 2) + 2 * half
        lower, upper = (cut, 2 * half + 2) if late else (2 * half, cut)
        lax.fori_loop(lower, upper, lambda n, c, refs=refs: prompt(n, c, *refs), 0)


def pair_kernel(keep, recv, out):
    pair = (keep[...].astype(F32) + recv[...].astype(F32)).astype(BF)
    out[...] = pair.reshape(CHIPS, SLICE, HD)


def scan_kernel(owners, pieces, out):
    core, chip, _, _ = place()
    home = owners[2 * core + chip // 16] // 2
    before = jnp.zeros((SLICE, HD), F32)
    for n in range(CHIPS):
        out[n, :SLICE] = before.astype(BF)
        before = before + pieces[n].astype(F32)
    total = before.astype(BF)
    nothing = jnp.zeros_like(total)
    for n in range(CHIPS):
        out[n, SLICE:] = jnp.where(home == n, total, nothing)


STATE = 2 * OWN * ROWS
LOW_ROWS = ROWS - LOW
WIDE = 2 * OWN * 64
NORMS = WIDE + 8
SENT = NORMS + 16


def prefix_kernel(back, keep, recv, own_o, other_o):
    before = back[:, :SLICE].reshape(STATE, HD).astype(F32)
    second = lax.axis_index("c") == 1
    added = jnp.where(second, recv[...], keep[...]).reshape(STATE, HD).astype(F32)
    both = (before + added).astype(BF)
    plain = before.astype(BF)
    own_o[...] = jnp.where(second, both, plain)
    other_o[:STATE] = jnp.where(second, plain, both)
    total = back[:, SLICE:].reshape(2 * OWN, ROWS, HD)
    other_o[STATE:] = total[:, LOW:].reshape(2 * OWN * LOW_ROWS, HD)


def norm_row(part):
    return jnp.concatenate([part[NORM : NORM + 1], part[NORM + 1 : NORM + 2, : ROWS - HD]], axis=1)


def spread_kernel(back, table, out):
    total = back[:, SLICE:].reshape(2 * OWN, ROWS, HD)
    for n in range(2 * OWN):
        wide = jnp.dot(table[...], total[n], preferred_element_type=F32).astype(BF)
        for f in range(4):
            out[f, n * 64 : (n + 1) * 64] = wide[f * 64 : (f + 1) * 64]
    norm = nt(jnp.concatenate([norm_row(total[n]) for n in range(2 * OWN)], axis=0), table[...])
    pad = jnp.zeros((8, 64), F32)
    for f in range(4):
        out[f, WIDE:NORMS] = jnp.concatenate([norm[:, f * 64 : (f + 1) * 64], pad], axis=1).astype(BF)


def attend(first, lens, state, num, den, feat, att_o):
    core, _, seq, _ = place()
    token = seq * SPAN + lax.broadcasted_iota(jnp.int32, (SPAN, HD), 0)
    ones = jnp.ones((8, HD), F32)
    found = []
    for n in range(2):
        live = token < lens[(first + n + 2 * core) % 4]
        den_all = den[first + n]
        squares = jnp.zeros((SPAN, HD), F32)
        for h in range(OWN):
            feats = feat[first + n, h]
            part = state(n, h)
            total = num[first + n, :, h * HD : (h + 1) * HD] + jnp.dot(feats, part, preferred_element_type=F32)
            below = nt(feats, jnp.broadcast_to(norm_row(part), (HD, ROWS))) + den_all[:, h : h + 1]
            att = jnp.where(live, total / below, 0.0)
            att_o[n, :, h * HD : (h + 1) * HD] = att
            squares = squares + att * att
        sums = lax.dot_general(
            ones,
            squares,
            (((1,), (1,)), ((), ())),
            precision=lax.Precision.HIGHEST,
            preferred_element_type=F32,
        )
        found += [sums[:1, :HD], sums[:1, HD:]]
    return found


def part_of(state):
    def part(n, h):
        at = (n * OWN + h) * ROWS
        return state[at : at + ROWS]

    return part


def own_kernel(
    lens, state, qa, ka, va, qb, kb, vb, picks, lines, num_i, den_i, feat_i,
    num, den, feat, att_o, square_o, quad_o, blank, sem
):
    blank[...] = jnp.zeros_like(blank)
    clear = [pltpu.make_async_copy(blank, quad_o.at[0, n], sem.at[n]) for n in range(4)]
    for copy in clear:
        copy.start()
    self_kernel(lens, (qa, ka, va), (qb, kb, vb), picks, lines, num, den, feat, late=True)
    found = attend(0, lens, part_of(state), num, den, feat, att_o)
    square_o[...] = jnp.concatenate(found + [jnp.zeros((4, HD), F32)], axis=0)
    for copy in clear:
        copy.wait()


def other_kernel(lens, state, num, den, feat, square, sent_i, att_o, sent_o):
    found = attend(2, lens, part_of(state), num, den, feat, att_o)
    squares = jnp.concatenate([square[:4]] + found, axis=0)
    high = squares.astype(BF)
    rest = (squares - high.astype(F32)).astype(BF)
    for f in range(4):
        sent_o[f, NORMS : NORMS + 8] = high
        sent_o[f, NORMS + 8 :] = rest


def mix_kernel(own, other, sent, mixed_o, block, sem):
    core = lax.axis_index("c")
    square = jnp.zeros((8, HD), F32)
    for f in range(4):
        square = square + (sent[f, NORMS : NORMS + 8].astype(F32) + sent[f, NORMS + 8 :].astype(F32))
    factor = lax.rsqrt(square * (1.0 / D) + NORM_FLOOR).T
    copies = []
    for local in range(4):
        source = own if local < 2 else other
        for k in range(2):
            column = factor[:, 2 * local + k : 2 * local + k + 1]
            rows = slice(k * HD, (k + 1) * HD)
            block[local, rows] = (source[local % 2, rows] * column).astype(BF)
        copies.append(pltpu.make_async_copy(block.at[local], mixed_o.at[(local + 2 * core) % 4], sem.at[local]))
        copies[-1].start()
    for copy in copies:
        copy.wait()


def final_kernel(
    owners, mine, theirs, low_mine, low_theirs, cleared, quad_o, low_o, nquad_o, nlow_o, block, low_b, nquad_b, nlow_b, sem
):
    core, _, seq, _ = place()
    low_b[...] = jnp.zeros_like(low_b)
    nquad_b[...] = jnp.zeros_like(nquad_b)
    nlow_b[...] = jnp.zeros_like(nlow_b)

    def move(local, f):
        heads = pl.ds(f * OWN, OWN)
        prompt = (local + 2 * core) % 4
        return pltpu.make_async_copy(block.at[local, heads], quad_o.at[0, prompt, heads], sem.at[local, f])

    for local in range(4):
        prompt = (local + 2 * core) % 4
        wide, low = (mine, low_mine) if local < 2 else (theirs, low_theirs)
        at = local % 2

        @pl.when(owners[prompt] == seq)
        def _():
            for f in range(4):
                for h in range(OWN):
                    row = (at * OWN + h) * 64
                    block[local, f * OWN + h] = wide[f, row : row + 64].astype(F32)
                move(local, f).start()
            for f in range(4):
                for h in range(OWN):
                    row = WIDE + at * OWN + h
                    nquad_b[prompt, f * OWN + h : f * OWN + h + 1] = wide[f, row : row + 1].astype(F32)[:, :64]
            for h in range(OWN):
                row = STATE + (at * OWN + h) * LOW_ROWS
                piece = low[row : row + LOW_ROWS].astype(F32)
                for r in range(FD + 1):
                    low_b[prompt, r, h : h + 1] = piece[r : r + 1]
                at_norm = NORM + 1 - LOW
                nlow_b[prompt, h : h + 1] = piece[at_norm : at_norm + 1, : FD + 1]

    small = [
        pltpu.make_async_copy(low_b, low_o.at[0], sem.at[4, 0]),
        pltpu.make_async_copy(nquad_b, nquad_o.at[0], sem.at[4, 1]),
        pltpu.make_async_copy(nlow_b, nlow_o.at[0], sem.at[4, 2]),
    ]
    for copy in small:
        copy.start()
    for local in range(4):

        @pl.when(owners[(local + 2 * core) % 4] == seq)
        def _():
            for f in range(4):
                move(local, f).wait()

    for copy in small:
        copy.wait()


SMEM = pl.BlockSpec(memory_space=pltpu.SMEM)
VMEM = pl.BlockSpec(memory_space=pltpu.VMEM)
ANY = pl.BlockSpec(memory_space=pl.ANY)
MIB = 1 << 20


def near(*arrays):
    return [pltpu.with_memory_space_constraint(a, pltpu.VMEM) for a in arrays]


def call(kernel, in_specs, out_shape, out_specs=None, grid=(), scratch=(), flops=0, limit=16, aliases=None):
    if out_specs is None:
        out_specs = jax.tree.map(lambda _: VMEM, out_shape, is_leaf=lambda x: not isinstance(x, (list, tuple)))
    return pl.pallas_call(
        kernel,
        grid=grid,
        in_specs=in_specs,
        out_specs=out_specs,
        out_shape=out_shape,
        scratch_shapes=scratch,
        input_output_aliases=aliases or {},
        cost_estimate=pl.CostEstimate(flops=flops, transcendentals=0, bytes_accessed=MIB),
        compiler_params=pltpu.CompilerParams(
            dimension_semantics=("arbitrary",) * len(grid), vmem_limit_bytes=limit * MIB
        ),
    )


def far(dims, dtype=BF):
    return jax.ShapeDtypeStruct(dims, dtype)


def shape(dims, dtype=BF):
    return pltpu.VMEM(dims, dtype)


def held(*arrays):
    return [pltpu.with_memory_space_constraint(a, pltpu.HBM) for a in arrays]


def body(hidden_in, w_query, w_key, w_value, lengths, owners):
    swap = [(0, 1), (1, 0)]
    half = (2, OWN * ROWS, HD)
    packed = OWN * ROWS

    rows = [shape((2, SPAN, 128)), shape((2, SPAN, 128)), shape((2, SPAN, 512)), shape(half)]
    qb, kb, vb, send, picks, hid, wv_b, wqk_b = call(
        project_kernel,
        [ANY] * 6,
        rows + [shape((2, packed, 128)), shape((4, SPAN, D)), shape((D, 512)), shape((D, 256))],
        scratch=[
            pltpu.SMEM((4,), jnp.int32),
            pltpu.SemaphoreType.DMA((D // CHUNK, 4)),
            pltpu.SemaphoreType.DMA((3,)),
            pltpu.SemaphoreType.DMA((2,)),
        ],
        flops=3_000_000_000,
        limit=24,
    )(*held(lengths, hidden_in, w_value, w_query, w_key, jnp.asarray(PICKS, BF)))

    recv = lax.ppermute(send, "c", swap)
    lines = jnp.asarray(LINES)
    own_shapes = [shape((4, SPAN, 512), F32), shape((4, SPAN, 128), F32), shape((4, OWN, SPAN, ROWS))]
    qa, ka, va, keep, num, den, feats = call(
        keep_kernel, [SMEM] + [VMEM] * 8, rows + own_shapes, flops=3_000_000_000, limit=24
    )(lengths, *near(hid, wqk_b, wv_b, picks, qb, kb, vb, lines))
    qkv = (qa, ka, va, qb, kb, vb)
    pair = call(pair_kernel, [VMEM, VMEM], shape((CHIPS, SLICE, HD)))(*near(keep, recv))
    pieces = lax.all_to_all(pair, CHIP, 0, 0)
    both = call(scan_kernel, [SMEM, VMEM], shape((CHIPS, 2 * SLICE, HD)))(owners, *near(pieces))
    back = lax.all_to_all(both, CHIP, 0, 0)
    own_state, given = call(
        prefix_kernel, [VMEM] * 3, [shape((STATE, HD)), shape((STATE + 2 * OWN * LOW_ROWS, HD))]
    )(*near(back, keep, recv))
    taken = lax.ppermute(given, "c", swap)
    num, den, feats, own_att, square, quad = call(
        own_kernel,
        [SMEM] + [VMEM] * 12,
        own_shapes + [shape((2, SPAN, 512), F32), shape((8, HD), F32), pltpu.HBM((1, 4, H, 64, HD), F32)],
        [VMEM] * 5 + [ANY],
        scratch=[pltpu.VMEM((H, 64, HD), F32), pltpu.SemaphoreType.DMA((4,))],
        flops=3_000_000_000,
        aliases={10: 0, 11: 1, 12: 2},
    )(lengths, *near(own_state, *qkv, picks, lines, num, den, feats))
    sent = call(spread_kernel, [VMEM] * 2, shape((4, SENT, HD)), flops=500_000_000)(
        *near(back, jnp.asarray(SPREAD, BF))
    )
    other_att, sent = call(
        other_kernel,
        [SMEM] + [VMEM] * 6,
        [shape((2, SPAN, 512), F32), shape((4, SENT, HD))],
        flops=500_000_000,
        aliases={6: 1},
    )(lengths, *near(taken, num, den, feats, square, sent))
    mine = lax.all_to_all(sent, "feat", 0, 0)
    theirs = lax.ppermute(mine, "c", swap)
    mixed = call(
        mix_kernel,
        [VMEM] * 3,
        pltpu.HBM((4, SPAN, 512), BF),
        ANY,
        scratch=[pltpu.VMEM((4, SPAN, 512), BF), pltpu.SemaphoreType.DMA((4,))],
        flops=500_000_000,
    )(*near(own_att, other_att, mine))

    quad, low_out, norm_quad, norm_low = call(
        final_kernel,
        [SMEM] + [VMEM] * 4 + [ANY],
        [
            pltpu.HBM((1, 4, H, 64, HD), F32),
            pltpu.HBM((1, 4, FD + 1, OWN, HD), F32),
            pltpu.HBM((1, 4, H, 64), F32),
            pltpu.HBM((1, 4, OWN, FD + 1), F32),
        ],
        [ANY] * 4,
        scratch=[
            pltpu.VMEM((4, H, 64, HD), F32),
            pltpu.VMEM((4, FD + 1, OWN, HD), F32),
            pltpu.VMEM((4, H, 64), F32),
            pltpu.VMEM((4, OWN, FD + 1), F32),
            pltpu.SemaphoreType.DMA((5, 4)),
        ],
        aliases={5: 0},
    )(owners, *near(mine, theirs, given, taken), *held(quad))
    return mixed, quad, jnp.transpose(low_out, (0, 1, 3, 2, 4)), norm_quad, norm_low


def solution(mesh):
    torus = Mesh(mesh.devices.reshape(8, 4, 2, 4), ("z", "y", "c", "feat"))
    seq = ("z", "y", "c")
    return jax.shard_map(
        body,
        mesh=torus,
        in_specs=(P(None, seq, None), P(), P(), P(None, "feat"), P(), P()),
        out_specs=(
            P(None, seq, "feat"),
            P(seq, None, None, "feat", None),
            P(seq, None, "feat", None, None),
            P(seq, None, None, "feat"),
            P(seq, None, "feat", None),
        ),
        check_vma=False,
    )
```

```python
import functools

import jax
import jax.numpy as jnp
import numpy as np
from jax import lax
from jax.experimental import pallas as pl
from jax.experimental.pallas import tpu as pltpu
from jax.sharding import Mesh
from jax.sharding import PartitionSpec as P

H = 16
FD = 16
HD = 128
D = 2048
SPAN = 256
OWN = 4
ROWS = 160
QUADS = 136
LOW = 128
NORM = 153
CHIPS = 32
SLICE = 2 * OWN * ROWS // CHIPS
NORM_FLOOR = 0.0001
BF = jnp.bfloat16
F32 = jnp.float32
CHIP = ("z", "y")


def feature_rows():
    pairs = [(i, j) for i in range(FD) for j in range(i, FD)]
    rows = [u if u < LOW else u + FD + 1 for u in range(QUADS)]
    return pairs, rows


def tables():
    pairs, rows = feature_rows()
    first = np.zeros((ROWS, FD), np.float32)
    second = np.zeros((ROWS, FD), np.float32)
    spread = np.zeros((FD * FD, ROWS), np.float32)
    for (i, j), row in zip(pairs, rows):
        first[row, i] = 1
        second[row, j] = 1
        spread[i * FD + j, row] = 1
        spread[j * FD + i, row] = 1
    for i in range(FD):
        first[LOW + 1 + i, i] = 1
    picks = np.zeros((2, 2, OWN, ROWS, 2 * OWN * FD), np.float32)
    for half in range(2):
        for head in range(OWN):
            at = half * OWN * FD + head * FD
            picks[half, 0, head, :, at : at + FD] = first
            picks[half, 1, head, :, at : at + FD] = second
    lines = np.zeros((8, ROWS), np.float32)
    for (i, j), row in zip(pairs, rows):
        lines[0, row] = (1.0 if i == j else 2.0) * (2.0 * FD) ** -0.5
    lines[0, LOW + 1 : LOW + 1 + FD] = lines[1, LOW + 1 : LOW + 1 + FD] = FD**-0.25
    lines[:3, LOW] = 1.0
    return picks.reshape(2, 2, OWN * ROWS, 2 * OWN * FD), spread, lines


PICKS, SPREAD, LINES = tables()


def is_low(row):
    return (row >= LOW) & (row <= LOW + FD)


def nt(a, b):
    return lax.dot_general(a, b, (((1,), (1,)), ((), ())), preferred_element_type=F32)


def place():
    core = lax.axis_index("c")
    chip = lax.axis_index("z") * 4 + lax.axis_index("y")
    return core, chip, chip * 2 + core, lax.axis_index("feat")


CHUNK = 512
AHEAD = 5


def project_kernel(lens_h, hid, wv, wq, wk, picks_h, q_o, k_o, v_o, send_o, picks, hid_b, wv_b, wqk_b, lens, sems, rest, small):
    core, _, seq, feat = place()
    lanes = pl.ds(pl.multiple_of(feat // 2 * 128, 128), 128)
    first = (2 + 2 * core) % 4
    queue = []
    for n in range(D // CHUNK):
        rows = pl.ds(n * CHUNK, CHUNK)
        queue.append(
            [
                pltpu.make_async_copy(hid.at[first, :, rows], hid_b.at[2, :, rows], sems.at[n, 0]),
                pltpu.make_async_copy(wq.at[rows, lanes], wqk_b.at[rows, :128], sems.at[n, 1]),
                pltpu.make_async_copy(wk.at[rows, lanes], wqk_b.at[rows, 128:], sems.at[n, 2]),
                pltpu.make_async_copy(wv.at[rows], wv_b.at[rows], sems.at[n, 3]),
            ]
        )
    queue.append(
        [
            pltpu.make_async_copy(lens_h, lens, small.at[0]),
            pltpu.make_async_copy(picks_h.at[feat % 2], picks, small.at[1]),
        ]
    )
    for n, local in enumerate((3, 0, 1)):
        queue.append([pltpu.make_async_copy(hid.at[(local + 2 * core) % 4], hid_b.at[local], rest.at[n])])

    def start(n):
        if n < len(queue):
            for copy in queue[n]:
                copy.start()

    def arrive(n):
        for copy in queue[n]:
            copy.wait()
        start(n + AHEAD)

    for n in range(AHEAD):
        start(n)
    def first_product():
        v = jnp.zeros((SPAN, 512), F32)
        qk = jnp.zeros((SPAN, 256), F32)
        for m in range(D // CHUNK):
            arrive(m)
            rows = slice(m * CHUNK, (m + 1) * CHUNK)
            x = hid_b[2, :, rows]
            qk = qk + jnp.dot(x, wqk_b[rows], preferred_element_type=F32)
            v = v + jnp.dot(x, wv_b[rows], preferred_element_type=F32)
        arrive(D // CHUNK)
        return qk, v

    keep_rows(0, first_product(), q_o, k_o, v_o)
    arrive(D // CHUNK + 1)
    keep_rows(1, product(hid_b[3], wqk_b, wv_b), q_o, k_o, v_o)
    states(0, 2, lens, k_o, v_o, picks, send_o)
    states(1, 3, lens, k_o, v_o, picks, send_o)
    for n in range(2, 4):
        arrive(D // CHUNK + n)


def product(x, wqk, wv):
    return (
        jnp.dot(x, wqk[...], preferred_element_type=F32),
        jnp.dot(x, wv[...], preferred_element_type=F32),
    )


def keep_rows(n, products, q_o, k_o, v_o):
    qk, v = products
    q_o[n] = qk[:, :128].astype(BF)
    k_o[n] = qk[:, 128:].astype(BF)
    v_o[n] = v.astype(BF)


def states(n, local, lens, k, v, picks, out):
    core, _, seq, _ = place()
    row = lax.broadcasted_iota(jnp.int32, (ROWS, SPAN), 0)
    low = is_low(row)
    const = (row == LOW).astype(F32)
    fixed = jnp.where(row == LOW, 1.0, jnp.where(low, FD**-0.25, (2.0 * FD) ** -0.5))
    ones = jnp.ones((8, SPAN), BF)
    tail_row = lax.broadcasted_iota(jnp.int32, (8, HD), 0) + (ROWS - 8)
    key_t = k[n].astype(F32).T.astype(BF)
    token = seq * SPAN + lax.broadcasted_iota(jnp.int32, (1, SPAN), 1)
    scale = jnp.where(token < lens[(local + 2 * core) % 4], fixed, 0.0)
    bias = jnp.where(low, scale, 0.0)
    for h in range(OWN):
        at = h * ROWS
        u = jnp.dot(picks[0, at : at + ROWS], key_t, preferred_element_type=F32)
        w = jnp.dot(picks[1, at : at + ROWS], key_t, preferred_element_type=F32)
        feats = ((u + const) * (w * scale + bias)).astype(BF)
        state = jnp.dot(feats, v[n, :, h * HD : (h + 1) * HD], preferred_element_type=F32)
        norm = nt(ones, feats)
        rest_norm = jnp.concatenate([norm[:, HD:], jnp.zeros((8, 2 * HD - ROWS), F32)], axis=1)
        tail = state[ROWS - 8 :]
        tail = jnp.where(tail_row == NORM, norm[:, :HD], jnp.where(tail_row == NORM + 1, rest_norm, tail))
        out[n, at : at + ROWS] = jnp.concatenate([state[: ROWS - 8], tail], axis=0).astype(BF)


def keep_kernel(
    lens, hid, wqk, wv, picks, qb, kb, vb, lines, qa, ka, va, keep_o, num_o, den_o, feat_o, quad_o, blank, sem
):
    blank[...] = jnp.zeros_like(blank)
    clear = [pltpu.make_async_copy(blank, quad_o.at[0, n], sem.at[n]) for n in range(4)]
    for copy in clear:
        copy.start()
    keep_rows(0, product(hid[0], wqk, wv), qa, ka, va)
    keep_rows(1, product(hid[1], wqk, wv), qa, ka, va)
    states(0, 0, lens, ka, va, picks, keep_o)
    states(1, 1, lens, ka, va, picks, keep_o)
    self_kernel(lens, (qa, ka, va), (qb, kb, vb), picks, lines, num_o, den_o, feat_o)
    for copy in clear:
        copy.wait()


def self_kernel(lens, own, other, picks, lines, num_o, den_o, feat_o, late=False):
    core, _, seq, feat = place()
    z = lax.axis_index("z")
    early = jnp.where(z < 4, 5 - z, 0) + (lax.axis_index("y") == 0).astype(jnp.int32)
    split = jnp.minimum(early, 4)
    tq = lax.broadcasted_iota(jnp.int32, (SPAN, SPAN), 0)
    tk = lax.broadcasted_iota(jnp.int32, (SPAN, SPAN), 1)
    lane = lax.broadcasted_iota(jnp.int32, (SPAN, HD), 1)
    scale, bias, const = lines[0:1], lines[1:2], lines[2:3]
    ones = jnp.ones((SPAN, HD), BF)

    def prompt(local, _, q, k, v):
        query = q[local % 2]
        key = k[local % 2]
        seen = (tk <= tq) & (seq * SPAN + tk < lens[(local + 2 * core) % 4])
        den_all = jnp.zeros((SPAN, HD), F32)
        for h in range(OWN):
            at = h * ROWS
            mine = jnp.where(lane // FD == feat % 2 * OWN + h, query, jnp.zeros_like(query))
            score = nt(mine, key)
            weight = jnp.where(seen, 1.0 + score * (FD**-0.5) + score * score * (0.5 / FD), 0.0).astype(BF)
            value = jnp.concatenate([v[local % 2, :, h * HD : (h + 1) * HD], ones], axis=1)
            both = jnp.dot(weight, value, preferred_element_type=F32)
            num_o[local, :, h * HD : (h + 1) * HD] = both[:, :HD]
            den_all = jnp.where(lane == h, both[:, HD:], den_all)
            u = nt(query, picks[0, at : at + ROWS])
            w = nt(query, picks[1, at : at + ROWS])
            feat_o[local, h] = ((u + const) * (w * scale + bias)).astype(BF)
        den_o[local] = den_all
        return _

    for half, refs in ((0, own), (1, other)):
        cut = jnp.clip(split - 2 * half, 0, 2) + 2 * half
        lower, upper = (cut, 2 * half + 2) if late else (2 * half, cut)
        lax.fori_loop(lower, upper, lambda n, c, refs=refs: prompt(n, c, *refs), 0)


def pair_kernel(keep, recv, out):
    pair = (keep[...].astype(F32) + recv[...].astype(F32)).astype(BF)
    out[...] = pair.reshape(CHIPS, SLICE, HD)


def scan_kernel(owners, pieces, out):
    core, chip, _, _ = place()
    home = owners[2 * core + chip // 16] // 2
    before = jnp.zeros((SLICE, HD), F32)
    for n in range(CHIPS):
        out[n, :SLICE] = before.astype(BF)
        before = before + pieces[n].astype(F32)
    total = before.astype(BF)
    nothing = jnp.zeros_like(total)
    for n in range(CHIPS):
        out[n, SLICE:] = jnp.where(home == n, total, nothing)


STATE = 2 * OWN * ROWS
LOW_ROWS = ROWS - LOW
WIDE = 2 * OWN * 64
NORMS = WIDE + 8
SENT = NORMS + 16


def prefix_kernel(back, keep, recv, own_o, other_o):
    before = back[:, :SLICE].reshape(STATE, HD).astype(F32)
    second = lax.axis_index("c") == 1
    added = jnp.where(second, recv[...], keep[...]).reshape(STATE, HD).astype(F32)
    both = (before + added).astype(BF)
    plain = before.astype(BF)
    own_o[...] = jnp.where(second, both, plain)
    other_o[:STATE] = jnp.where(second, plain, both)
    total = back[:, SLICE:].reshape(2 * OWN, ROWS, HD)
    other_o[STATE:] = total[:, LOW:].reshape(2 * OWN * LOW_ROWS, HD)


def norm_row(part):
    return jnp.concatenate([part[NORM : NORM + 1], part[NORM + 1 : NORM + 2, : ROWS - HD]], axis=1)


def spread_kernel(back, table, out):
    total = back[:, SLICE:].reshape(2 * OWN, ROWS, HD)
    for n in range(2 * OWN):
        wide = jnp.dot(table[...], total[n], preferred_element_type=F32).astype(BF)
        for f in range(4):
            out[f, n * 64 : (n + 1) * 64] = wide[f * 64 : (f + 1) * 64]
    norm = nt(jnp.concatenate([norm_row(total[n]) for n in range(2 * OWN)], axis=0), table[...])
    pad = jnp.zeros((8, 64), F32)
    for f in range(4):
        out[f, WIDE:NORMS] = jnp.concatenate([norm[:, f * 64 : (f + 1) * 64], pad], axis=1).astype(BF)


def attend(first, lens, state, num, den, feat, att_o):
    core, _, seq, _ = place()
    token = seq * SPAN + lax.broadcasted_iota(jnp.int32, (SPAN, HD), 0)
    ones = jnp.ones((8, HD), F32)
    found = []
    for n in range(2):
        live = token < lens[(first + n + 2 * core) % 4]
        den_all = den[first + n]
        squares = jnp.zeros((SPAN, HD), F32)
        for h in range(OWN):
            feats = feat[first + n, h]
            part = state(n, h)
            total = num[first + n, :, h * HD : (h + 1) * HD] + jnp.dot(feats, part, preferred_element_type=F32)
            below = nt(feats, jnp.broadcast_to(norm_row(part), (HD, ROWS))) + den_all[:, h : h + 1]
            att = jnp.where(live, total / below, 0.0)
            att_o[n, :, h * HD : (h + 1) * HD] = att
            squares = squares + att * att
        sums = lax.dot_general(
            ones,
            squares,
            (((1,), (1,)), ((), ())),
            precision=lax.Precision.HIGHEST,
            preferred_element_type=F32,
        )
        found += [sums[:1, :HD], sums[:1, HD:]]
    return found


def part_of(state):
    def part(n, h):
        at = (n * OWN + h) * ROWS
        return state[at : at + ROWS]

    return part


def own_kernel(
    lens, state, qa, ka, va, qb, kb, vb, picks, lines, num_i, den_i, feat_i, back, table,
    num, den, feat, att_o, square_o, sent_o
):
    spread_kernel(back, table, sent_o)
    self_kernel(lens, (qa, ka, va), (qb, kb, vb), picks, lines, num, den, feat, late=True)
    found = attend(0, lens, part_of(state), num, den, feat, att_o)
    square_o[...] = jnp.concatenate(found + [jnp.zeros((4, HD), F32)], axis=0)


def other_kernel(lens, state, num, den, feat, square, sent_i, att_o, sent_o):
    found = attend(2, lens, part_of(state), num, den, feat, att_o)
    squares = jnp.concatenate([square[:4]] + found, axis=0)
    high = squares.astype(BF)
    rest = (squares - high.astype(F32)).astype(BF)
    for f in range(4):
        sent_o[f, NORMS : NORMS + 8] = high
        sent_o[f, NORMS + 8 :] = rest


def mix_kernel(own, other, sent, mixed_o, block, sem):
    core = lax.axis_index("c")
    square = jnp.zeros((8, HD), F32)
    for f in range(4):
        square = square + (sent[f, NORMS : NORMS + 8].astype(F32) + sent[f, NORMS + 8 :].astype(F32))
    factor = lax.rsqrt(square * (1.0 / D) + NORM_FLOOR).T
    copies = []
    for local in range(4):
        source = own if local < 2 else other
        for k in range(2):
            column = factor[:, 2 * local + k : 2 * local + k + 1]
            rows = slice(k * HD, (k + 1) * HD)
            block[local, rows] = (source[local % 2, rows] * column).astype(BF)
        copies.append(pltpu.make_async_copy(block.at[local], mixed_o.at[(local + 2 * core) % 4], sem.at[local]))
        copies[-1].start()
    for copy in copies:
        copy.wait()


def final_kernel(
    owners, mine, theirs, low_mine, low_theirs, cleared, quad_o, low_o, nquad_o, nlow_o, block, low_b, nquad_b, nlow_b, sem
):
    core, _, seq, _ = place()
    low_b[...] = jnp.zeros_like(low_b)
    nquad_b[...] = jnp.zeros_like(nquad_b)
    nlow_b[...] = jnp.zeros_like(nlow_b)

    def move(local, f):
        heads = pl.ds(f * OWN, OWN)
        prompt = (local + 2 * core) % 4
        return pltpu.make_async_copy(block.at[local, heads], quad_o.at[0, prompt, heads], sem.at[local, f])

    for local in range(4):
        prompt = (local + 2 * core) % 4
        wide, low = (mine, low_mine) if local < 2 else (theirs, low_theirs)
        at = local % 2

        @pl.when(owners[prompt] == seq)
        def _():
            for f in range(4):
                for h in range(OWN):
                    row = (at * OWN + h) * 64
                    block[local, f * OWN + h] = wide[f, row : row + 64].astype(F32)
                move(local, f).start()
            for f in range(4):
                for h in range(OWN):
                    row = WIDE + at * OWN + h
                    nquad_b[prompt, f * OWN + h : f * OWN + h + 1] = wide[f, row : row + 1].astype(F32)[:, :64]
            for h in range(OWN):
                row = STATE + (at * OWN + h) * LOW_ROWS
                piece = low[row : row + LOW_ROWS].astype(F32)
                for r in range(FD + 1):
                    low_b[prompt, r, h : h + 1] = piece[r : r + 1]
                at_norm = NORM + 1 - LOW
                nlow_b[prompt, h : h + 1] = piece[at_norm : at_norm + 1, : FD + 1]

    small = [
        pltpu.make_async_copy(low_b, low_o.at[0], sem.at[4, 0]),
        pltpu.make_async_copy(nquad_b, nquad_o.at[0], sem.at[4, 1]),
        pltpu.make_async_copy(nlow_b, nlow_o.at[0], sem.at[4, 2]),
    ]
    for copy in small:
        copy.start()
    for local in range(4):

        @pl.when(owners[(local + 2 * core) % 4] == seq)
        def _():
            for f in range(4):
                move(local, f).wait()

    for copy in small:
        copy.wait()


SMEM = pl.BlockSpec(memory_space=pltpu.SMEM)
VMEM = pl.BlockSpec(memory_space=pltpu.VMEM)
ANY = pl.BlockSpec(memory_space=pl.ANY)
MIB = 1 << 20


def near(*arrays):
    return [pltpu.with_memory_space_constraint(a, pltpu.VMEM) for a in arrays]


def call(kernel, in_specs, out_shape, out_specs=None, grid=(), scratch=(), flops=0, limit=16, aliases=None):
    if out_specs is None:
        out_specs = jax.tree.map(lambda _: VMEM, out_shape, is_leaf=lambda x: not isinstance(x, (list, tuple)))
    return pl.pallas_call(
        kernel,
        grid=grid,
        in_specs=in_specs,
        out_specs=out_specs,
        out_shape=out_shape,
        scratch_shapes=scratch,
        input_output_aliases=aliases or {},
        cost_estimate=pl.CostEstimate(flops=flops, transcendentals=0, bytes_accessed=MIB),
        compiler_params=pltpu.CompilerParams(
            dimension_semantics=("arbitrary",) * len(grid), vmem_limit_bytes=limit * MIB
        ),
    )


def far(dims, dtype=BF):
    return jax.ShapeDtypeStruct(dims, dtype)


def shape(dims, dtype=BF):
    return pltpu.VMEM(dims, dtype)


def held(*arrays):
    return [pltpu.with_memory_space_constraint(a, pltpu.HBM) for a in arrays]


def body(hidden_in, w_query, w_key, w_value, lengths, owners):
    swap = [(0, 1), (1, 0)]
    half = (2, OWN * ROWS, HD)
    packed = OWN * ROWS

    rows = [shape((2, SPAN, 128)), shape((2, SPAN, 128)), shape((2, SPAN, 512)), shape(half)]
    qb, kb, vb, send, picks, hid, wv_b, wqk_b = call(
        project_kernel,
        [ANY] * 6,
        rows + [shape((2, packed, 128)), shape((4, SPAN, D)), shape((D, 512)), shape((D, 256))],
        scratch=[
            pltpu.SMEM((4,), jnp.int32),
            pltpu.SemaphoreType.DMA((D // CHUNK, 4)),
            pltpu.SemaphoreType.DMA((3,)),
            pltpu.SemaphoreType.DMA((2,)),
        ],
        flops=3_000_000_000,
        limit=24,
    )(*held(lengths, hidden_in, w_value, w_query, w_key, jnp.asarray(PICKS, BF)))

    recv = lax.ppermute(send, "c", swap)
    lines = jnp.asarray(LINES)
    own_shapes = [shape((4, SPAN, 512), F32), shape((4, SPAN, 128), F32), shape((4, OWN, SPAN, ROWS))]
    qa, ka, va, keep, num, den, feats, quad = call(
        keep_kernel,
        [SMEM] + [VMEM] * 8,
        rows + own_shapes + [pltpu.HBM((1, 4, H, 64, HD), F32)],
        [VMEM] * 7 + [ANY],
        scratch=[pltpu.VMEM((H, 64, HD), F32), pltpu.SemaphoreType.DMA((4,))],
        flops=3_000_000_000,
        limit=24,
    )(lengths, *near(hid, wqk_b, wv_b, picks, qb, kb, vb, lines))
    qkv = (qa, ka, va, qb, kb, vb)
    pair = call(pair_kernel, [VMEM, VMEM], shape((CHIPS, SLICE, HD)))(*near(keep, recv))
    pieces = lax.all_to_all(pair, CHIP, 0, 0)
    both = call(scan_kernel, [SMEM, VMEM], shape((CHIPS, 2 * SLICE, HD)))(owners, *near(pieces))
    back = lax.all_to_all(both, CHIP, 0, 0)
    own_state, given = call(
        prefix_kernel, [VMEM] * 3, [shape((STATE, HD)), shape((STATE + 2 * OWN * LOW_ROWS, HD))]
    )(*near(back, keep, recv))
    taken = lax.ppermute(given, "c", swap)
    num, den, feats, own_att, square, sent = call(
        own_kernel,
        [SMEM] + [VMEM] * 14,
        own_shapes + [shape((2, SPAN, 512), F32), shape((8, HD), F32), shape((4, SENT, HD))],
        flops=3_000_000_000,
        aliases={10: 0, 11: 1, 12: 2},
    )(lengths, *near(own_state, *qkv, picks, lines, num, den, feats, back, jnp.asarray(SPREAD, BF)))
    other_att, sent = call(
        other_kernel,
        [SMEM] + [VMEM] * 6,
        [shape((2, SPAN, 512), F32), shape((4, SENT, HD))],
        flops=500_000_000,
        aliases={6: 1},
    )(lengths, *near(taken, num, den, feats, square, sent))
    mine = lax.all_to_all(sent, "feat", 0, 0)
    theirs = lax.ppermute(mine, "c", swap)
    mixed = call(
        mix_kernel,
        [VMEM] * 3,
        pltpu.HBM((4, SPAN, 512), BF),
        ANY,
        scratch=[pltpu.VMEM((4, SPAN, 512), BF), pltpu.SemaphoreType.DMA((4,))],
        flops=500_000_000,
    )(*near(own_att, other_att, mine))

    quad, low_out, norm_quad, norm_low = call(
        final_kernel,
        [SMEM] + [VMEM] * 4 + [ANY],
        [
            pltpu.HBM((1, 4, H, 64, HD), F32),
            pltpu.HBM((1, 4, FD + 1, OWN, HD), F32),
            pltpu.HBM((1, 4, H, 64), F32),
            pltpu.HBM((1, 4, OWN, FD + 1), F32),
        ],
        [ANY] * 4,
        scratch=[
            pltpu.VMEM((4, H, 64, HD), F32),
            pltpu.VMEM((4, FD + 1, OWN, HD), F32),
            pltpu.VMEM((4, H, 64), F32),
            pltpu.VMEM((4, OWN, FD + 1), F32),
            pltpu.SemaphoreType.DMA((5, 4)),
        ],
        aliases={5: 0},
    )(owners, *near(mine, theirs, given, taken), *held(quad))
    return mixed, quad, jnp.transpose(low_out, (0, 1, 3, 2, 4)), norm_quad, norm_low


def solution(mesh):
    torus = Mesh(mesh.devices.reshape(8, 4, 2, 4), ("z", "y", "c", "feat"))
    seq = ("z", "y", "c")
    return jax.shard_map(
        body,
        mesh=torus,
        in_specs=(P(None, seq, None), P(), P(), P(None, "feat"), P(), P()),
        out_specs=(
            P(None, seq, "feat"),
            P(seq, None, None, "feat", None),
            P(seq, None, "feat", None, None),
            P(seq, None, None, "feat"),
            P(seq, None, "feat", None),
        ),
        check_vma=False,
    )
```
